32 devices in a mesh: gx: 4 (over z), gy: 4 (over y, core), gz: 2 (over x).
Axes of the slice: x: 2, y: 2, z: 4, core: 2. Of those that a mesh axis runs over, the one named last changes fastest.
Arguments:
- coarse_source: float32 [64, 128, 256], P('gx', 'gy', 'gz'), may hold values from -6 to 6
- coarse_shift: float32 [64, 128, 256], P('gx', 'gy', 'gz'), may hold values from 0.1 to 4
- coarse_start: float32 [64, 128, 256], P('gx', 'gy', 'gz'), may hold values from -3 to 3
- fine_source: float32 [128, 32768], P(('gx', 'gy', 'gz')), may hold values from -6 to 6
- fine_shift: float32 [128, 32768], P(('gx', 'gy', 'gz')), may hold values from 0.1 to 4
- fine_start: float32 [128, 32768], P(('gx', 'gy', 'gz')), may hold values from -3 to 3
- box_corner: int32 [32, 4, 3], P(('gx', 'gy', 'gz')), may hold values from 0 to 480, as said below
- box_owner: int32 [32, 4], P(('gx', 'gy', 'gz')), may hold values from 0 to 8, as said below
Outputs:
- potential: float32 [64, 128, 256], P('gx', 'gy', 'gz')
- fine_solution: float32 [128, 32768], P(('gx', 'gy', 'gz'))
- residual_norms: float32 [2], replicated
The draws below stay inside these ranges and needn't reach their ends.
Inputs may be any that keep to these rules, and one draw needn't show every extreme that they name: `box_owner`: each device has at least one live slot; in every group of 8 devices that share a gx index some device has 4 live slots; the live owners of one device are distinct; no device is the owner of more than 4 live boxes, and in every group some device is the owner of exactly 4 live boxes. `box_corner`: each corner is a multiple of 32 and its footprint lies in the coarse block of the device that lists it; the 4 footprints of one device are distinct.
All inputs are finite; a program needn't handle non-finite values.
Results may differ from the reference program's by a relative error of at most 0.0001.
Values sent between devices are 32-bit elements; how exact they have to be, the bound alone decides.
A program may use at most 128 MiB of HBM per device.

```python
import math
import jax
import jax.numpy as jnp
from jax import lax

CX = 16
CY = 32
CZ = 128
FOOT = 16
SLOTS = 4
CYCLES = 2
CSWEEPS = 4
FSWEEPS = 3
FINE = 32768
BOXES = 128
NX = 64
NY = 128
NZ = 256
N_GY = 4
N_GZ = 2
DEVICES = 32


def draw_box_owner(key, part):
    group = N_GY * N_GZ
    keys = jax.random.split(jax.random.fold_in(key, 41), DEVICES // group)

    def choose(single):
        return jax.random.permutation(single, group)[:SLOTS].astype(jnp.int32)
    offsets = jnp.repeat(jax.vmap(choose)(keys), group, axis=0)
    heavy = jnp.repeat(jax.random.randint(jax.random.fold_in(key, 42), (DEVICES // group,), 0, group).astype(jnp.int32), group)
    counts = jax.random.randint(jax.random.fold_in(key, 11), (DEVICES,), 1, SLOTS + 1).astype(jnp.int32)
    rank = jnp.arange(DEVICES, dtype=jnp.int32) % group
    senders = (heavy[:, None] - offsets) % group
    full = jnp.any(senders == rank[:, None], axis=1)
    counts = jnp.where(full, SLOTS, counts).astype(jnp.int32)
    owners = ((rank[:, None] + offsets) % group).astype(jnp.int32)
    slot = jnp.arange(SLOTS, dtype=jnp.int32)[None, :]
    return jnp.where(slot < counts[:, None], owners, group).astype(jnp.int32)


def draw_box_corner(key, part):
    group = N_GY * N_GZ
    along_x = CX // FOOT
    along_y = CY // FOOT
    along_z = CZ // FOOT
    places = along_x * along_y * along_z
    keys = jax.random.split(jax.random.fold_in(key, 31), DEVICES)

    def choose(single):
        return jax.random.permutation(single, places)[:SLOTS].astype(jnp.int32)
    picked = jax.vmap(choose)(keys)
    device = jnp.arange(DEVICES, dtype=jnp.int32)[:, None]
    device_x = device // group
    device_y = device // N_GZ % N_GY
    device_z = device % N_GZ
    block_x = picked // (along_y * along_z)
    block_y = picked // along_z % along_y
    block_z = picked % along_z
    fine_x = 2 * (device_x * CX + block_x * FOOT)
    fine_y = 2 * (device_y * CY + block_y * FOOT)
    fine_z = 2 * (device_z * CZ + block_z * FOOT)
    return jnp.stack([fine_x, fine_y, fine_z], axis=-1).astype(jnp.int32)


def block_levels(stream_key, dims, shards, low, largest):
    loudness = 1.0
    for axis_at, blocks in shards:
        steps = jax.random.uniform(jax.random.fold_in(jax.random.fold_in(stream_key, 6), axis_at), (blocks,), jnp.float32, low / len(shards), largest / len(shards))
        loudness = loudness * jnp.repeat(jnp.exp(steps), dims[axis_at] // blocks).reshape((-1,) + (1,) * (len(dims) - 1 - axis_at))
    return loudness


def noise(rng, dims, deviation, limit, cuts=(), kind=jnp.bfloat16):
    result = jax.random.normal(rng, dims, jnp.float32) * deviation
    if len(cuts) > 0:
        result = block_levels(rng, dims, cuts, -0.22, 0.18) * result
    return jnp.clip(result, min=-limit, max=limit).astype(kind)


def setup_inputs(seed: int = 0) -> dict:
    seeds = jax.random.split(jax.random.key(seed), 9)
    coarse_source = noise(seeds[0], (NX, NY, NZ), 1.0, 6.0, ((0, 4), (1, 4), (2, 2)), jnp.float32)
    coarse_shift = jnp.clip(jnp.exp(math.log(4.0) - 3.6888794 * jax.random.uniform(seeds[1], (NX, NY, NZ), jnp.float32) ** block_levels(seeds[1], (NX, NY, NZ), ((0, 4), (1, 4), (2, 2)), -0.2, 0.2)), 0.1, 4.0)
    coarse_start = noise(seeds[2], (NX, NY, NZ), 0.5, 3.0, ((0, 4), (1, 4), (2, 2)), jnp.float32)
    fine_source = noise(seeds[3], (BOXES, FINE), 1.0, 6.0, ((0, 32),), jnp.float32)
    fine_shift = jnp.clip(jnp.exp(math.log(4.0) - 3.6888794 * jax.random.uniform(seeds[4], (BOXES, FINE), jnp.float32) ** block_levels(seeds[4], (BOXES, FINE), ((0, 32),), -0.2, 0.2)), 0.1, 4.0)
    fine_start = noise(seeds[5], (BOXES, FINE), 0.5, 3.0, ((0, 32),), jnp.float32)
    box_corner = draw_box_corner(jax.random.fold_in(seeds[8], 71), 0)
    box_owner = draw_box_owner(jax.random.fold_in(seeds[8], 71), 0)
    return {"coarse_source": coarse_source, "coarse_shift": coarse_shift, "coarse_start": coarse_start, "fine_source": fine_source, "fine_shift": fine_shift, "fine_start": fine_start, "box_corner": box_corner, "box_owner": box_owner}


OMEGA = 0.8

def to_blocks(field):
    extent = field.shape
    shaped = field.reshape(extent[0] // FOOT, FOOT, extent[1] // FOOT, FOOT, extent[2] // FOOT, FOOT)
    return shaped.transpose(0, 2, 4, 1, 3, 5).reshape(-1, FOOT * FOOT * FOOT)

def from_blocks(blocks, extent):
    shaped = blocks.reshape(extent[0] // FOOT, extent[1] // FOOT, extent[2] // FOOT, FOOT, FOOT, FOOT)
    return shaped.transpose(0, 3, 1, 4, 2, 5).reshape(extent)

def inject(parents):
    number = parents.shape[0]
    shaped = parents.reshape(number, FOOT, 1, FOOT, 1, FOOT, 1)
    spread = jnp.broadcast_to(shaped, (number, FOOT, 2, FOOT, 2, FOOT, 2))
    return spread.reshape(number, 8 * FOOT * FOOT * FOOT)

def restrict(values):
    number = values.shape[0]
    return values.reshape(number, FOOT, 2, FOOT, 2, FOOT, 2).mean(axis=(2, 4, 6)).reshape(number, FOOT * FOOT * FOOT)

def fine_residual(values, parents, source, shift):
    ghost = inject(parents)
    side = 2 * FOOT
    position = jnp.arange(side * side * side, dtype=jnp.int32)[None, :]
    summed = jnp.zeros_like(values)
    for stride in (1, side, side * side):
        coordinate = position // stride % side
        upper = jnp.roll(values, -stride, axis=1)
        lower = jnp.roll(values, stride, axis=1)
        summed = summed + jnp.where(coordinate < side - 1, upper, ghost) + jnp.where(coordinate > 0, lower, ghost)
    return source - (6.0 + shift) * values + summed

def beside_sum(padded):
    summed = padded[2:, 1:-1, 1:-1] + padded[:-2, 1:-1, 1:-1]
    summed = summed + padded[1:-1, 2:, 1:-1] + padded[1:-1, :-2, 1:-1]
    return summed + padded[1:-1, 1:-1, 2:] + padded[1:-1, 1:-1, :-2]

def reference(coarse_source, coarse_shift, coarse_start, fine_source, fine_shift, fine_start, box_corner, box_owner):
    group = N_GY * N_GZ
    device_ids = jnp.arange(DEVICES, dtype=jnp.int32)
    live = box_owner < group
    owner_safe = jnp.minimum(box_owner, group - 1).astype(jnp.int32)
    hit = ((box_owner[:, :, None] == jnp.arange(group, dtype=jnp.int32)[None, None, :]) & live[:, :, None]).astype(jnp.int32)
    incoming = lax.optimization_barrier(jnp.sum(hit, axis=1)).astype(jnp.int32)
    grouped = incoming.reshape(DEVICES // group, group, group)
    before = (jnp.cumsum(grouped, axis=1).astype(jnp.int32) - grouped).reshape(DEVICES, group).astype(jnp.int32)
    slot_j = jnp.take_along_axis(before, owner_safe, axis=1).astype(jnp.int32)
    owner_global = ((device_ids // group)[:, None] * group + owner_safe).astype(jnp.int32)
    rows = (owner_global * SLOTS + slot_j).astype(jnp.int32)
    targets = jnp.where(live, rows, BOXES).reshape(-1).astype(jnp.int32)
    block = (box_corner // 2 // FOOT).reshape(-1, 3)
    block_index = ((block[:, 0] * (NY // FOOT) + block[:, 1]) * (NZ // FOOT) + block[:, 2]).astype(jnp.int32)
    home_of_row = jnp.zeros((BOXES,), jnp.int32).at[targets].set(jnp.arange(DEVICES * SLOTS, dtype=jnp.int32), mode='drop')
    occupied = jnp.zeros((BOXES,), jnp.float32).at[targets].set(1.0, mode='drop')[:, None]
    row_block = block_index[home_of_row].astype(jnp.int32)
    source = fine_source
    shift = fine_shift
    values = fine_start
    fine_diagonal = 6.0 + shift
    diagonal = 6.0 + coarse_shift
    potential = coarse_start
    earlier = None
    norms = []
    for cycle in range(CYCLES):
        parents = to_blocks(potential)[row_block]
        if cycle > 0:
            values = values + inject(parents - earlier)
        for sweep in range(FSWEEPS):
            values = values + OMEGA * fine_residual(values, parents, source, shift) / fine_diagonal
        remainder = fine_residual(values, parents, source, shift)
        restricted = restrict(remainder) * occupied
        placed = jnp.zeros((NX // FOOT * (NY // FOOT) * (NZ // FOOT), FOOT * FOOT * FOOT), jnp.float32)
        placed = placed.at[row_block].add(restricted)
        composite = coarse_source + from_blocks(placed, coarse_source.shape)
        for sweep in range(CSWEEPS):
            residual = composite - diagonal * potential + beside_sum(jnp.pad(potential, 1))
            potential = potential + OMEGA * residual / diagonal
        squares = jnp.sum(residual * residual) + jnp.sum(occupied * remainder * remainder)
        norms.append(jnp.sqrt(squares / (NX * NY * NZ)))
        earlier = parents
    parents = to_blocks(potential)[row_block]
    fine_solution = (values + inject(parents - earlier)) * occupied
    return (potential, fine_solution, jnp.stack(norms))
```

```python
import functools

import jax
import jax.numpy as jnp
from jax import lax
from jax.experimental import pallas as pl
from jax.experimental.pallas import tpu as pltpu
from jax.sharding import PartitionSpec as P

FOOT = 16
CYCLES = 2
CSWEEPS = 4
FSWEEPS = 3
OMEGA = 0.8
KEEP = 1.0 - OMEGA
MESH = pl.DeviceIdType.MESH
LANES = 128
SIDE = 2 * FOOT


def take(x, idx):
    return jnp.take_along_axis(x, idx, axis=1, mode="promise_in_bounds")


def iota(shape, dim):
    return lax.broadcasted_iota(jnp.int32, shape, dim)


def kernel(
    sizes,
    corner,
    owner,
    c_src_hbm,
    c_shift_hbm,
    c_start_hbm,
    f_src_hbm,
    f_shift_hbm,
    f_start_hbm,
    pot_out,
    fine_out,
    norm_out,
    c_src,
    c_shift,
    f_src,
    f_shift,
    f_start,
    in_sem,
    U,
    W,
    comp,
    yh,
    ys,
    zh,
    zs,
    V,
    FW,
    FS,
    FD,
    G,
    compact,
    R,
    pout,
    prec,
    rout,
    rrec,
    slotid,
    sums,
    xsum,
    p_send,
    p_recv,
    r_send,
    r_recv,
    h_send,
    h_recv,
    n_send,
    n_recv,
):
    n_gx, n_gy, n_gz = sizes
    group = n_gy * n_gz
    slots = owner.shape[1]
    nx, ny, nz = c_src_hbm.shape
    along_y = ny // FOOT
    gx, gy, gz = lax.axis_index("gx"), lax.axis_index("gy"), lax.axis_index("gz")
    me = gy * n_gz + gz

    def rank_id(rank):
        return (gx, rank // n_gz, rank % n_gz)

    have = (gx > 0, gx < n_gx - 1, gy > 0, gy < n_gy - 1, gz > 0, gz < n_gz - 1)
    beside = (
        (gx - 1, gy, gz),
        (gx + 1, gy, gz),
        (gx, gy - 1, gz),
        (gx, gy + 1, gz),
        (gx, gy, gz - 1),
        (gx, gy, gz + 1),
    )

    loads = [
        pltpu.make_async_copy(source, target, in_sem.at[i])
        for i, (source, target) in enumerate(
            (
                (c_start_hbm, U.at[0, pl.ds(1, nx)]),
                (c_shift_hbm, c_shift),
                (f_start_hbm, f_start),
                (f_src_hbm, f_src),
                (f_shift_hbm, f_shift),
                (c_src_hbm, c_src),
            )
        )
    ]
    for load in loads:
        load.start()

    for p in range(2):
        U[p, 0] = jnp.zeros((ny, nz), jnp.float32)
        U[p, nx + 1] = jnp.zeros((ny, nz), jnp.float32)
    yh[...] = jnp.zeros_like(yh)
    zh[...] = jnp.zeros_like(zh)

    barrier = pltpu.get_barrier_semaphore()
    for d in range(1, group):
        pl.semaphore_signal(barrier, inc=1, device_id=rank_id((me + d) % group), device_id_type=MESH)
    for d in range(1, n_gx):
        pl.semaphore_signal(barrier, inc=1, device_id=((gx + d) % n_gx, gy, gz), device_id_type=MESH)
    pl.semaphore_wait(barrier, group - 1 + n_gx - 1)

    tile = (8, LANES)
    lane = iota(tile, 1)
    sub = iota(tile, 0)
    wide = (ny, LANES)
    wlane = iota(wide, 1)
    wsub = iota(wide, 0)
    box_row = []
    box_col = []
    box_live = []
    for s in range(slots):
        box_row.append((corner[1, 0, s] // 2 - gy * ny) // FOOT)
        box_col.append((corner[2, 0, s] // 2 - gz * nz) // FOOT)
        box_live.append(owner[0, s] < group)

    def exchange(out, rec, send, recv, rows):
        copies = []
        for d in range(1, group):
            peer = (me + d) % group
            copy = pltpu.make_async_remote_copy(
                src_ref=out.at[peer, pl.ds(0, rows)],
                dst_ref=rec.at[me, pl.ds(0, rows)],
                send_sem=send.at[d],
                recv_sem=recv.at[d],
                device_id=rank_id(peer),
                device_id_type=MESH,
            )
            copy.start()
            copies.append(copy)
        rec[me, pl.ds(0, rows)] = out[me, pl.ds(0, rows)]
        return copies

    def arrive(out, rec, send, recv, rows):
        for d in range(1, group):
            source = (me + group - d) % group
            pltpu.make_async_remote_copy(
                src_ref=out.at[source, pl.ds(0, rows)],
                dst_ref=rec.at[source, pl.ds(0, rows)],
                send_sem=send.at[d],
                recv_sem=recv.at[d],
                device_id=rank_id(source),
                device_id_type=MESH,
            ).wait_recv()

    def pack_parents(p):
        @pl.loop(0, FOOT // 4)
        def _(xg):
            for s in range(slots):
                idx = box_col[s] * FOOT + (lane % FOOT)
                acc = jnp.zeros(tile, jnp.float32)
                for k in range(4):
                    for yl in range(2):
                        a = U[p, 1 + xg * 4 + k, pl.ds(yl, 8, stride=2), :]
                        for b in range(1, along_y):
                            other = U[p, 1 + xg * 4 + k, pl.ds(b * FOOT + yl, 8, stride=2), :]
                            a = jnp.where(box_row[s] == b, other, a)
                        acc = jnp.where(lane // FOOT == 2 * k + yl, take(a, idx), acc)
                compact[s, pl.ds(pl.multiple_of(xg * 8, 8), 8), :] = acc

        for q in range(group):
            acc = jnp.zeros((32, LANES), jnp.float32)
            flag = jnp.zeros(tile, jnp.float32)
            for s in range(slots):
                acc = jnp.where(owner[0, s] == q, compact[s], acc)
                flag = jnp.where(owner[0, s] == q, 1.0, flag)
            pout[q, pl.ds(0, 32)] = acc
            pout[q, pl.ds(32, 8)] = flag

    def slot_masks():
        count = jnp.zeros(tile, jnp.float32)
        for q in range(group):
            flag = prec[q, pl.ds(32, 8)]
            slotid[q] = jnp.where(flag > 0.5, count, -1.0)
            count = count + flag
        return count

    spread_lane = (lane // 64) * FOOT + (lane % SIDE) // 2

    def ghosts(par):
        @pl.loop(0, FOOT // 4)
        def _(xg):
            rows = pl.ds(pl.multiple_of(xg * 8, 8), 8)
            for j in range(slots):
                acc = jnp.zeros(tile, jnp.float32)
                for q in range(group):
                    acc = jnp.where(slotid[q] == float(j), prec[q, rows], acc)
                for k in range(4):
                    G[par, j, xg * 4 + k] = take(acc, k * SIDE + spread_lane)

    y_top = (lane >= 96) & (sub == 7)
    y_low = (lane < 32) & (sub == 0)
    z_pos = lane % SIDE

    def plane(x, shift=0):
        start = pl.multiple_of((x + 1) * 8, 8)
        return pl.ds(start + shift, 8)

    def beside_fine(vp, par, j, x, ghost):
        v = V[vp, j, plane(x)]
        up = jnp.where(lane < 32, V[vp, j, plane(x, 1)], v)
        up = jnp.where(y_top, ghost, pltpu.roll(up, LANES - 32, 1))
        lo = jnp.where(lane >= 96, V[vp, j, plane(x, -1)], v)
        lo = jnp.where(y_low, ghost, pltpu.roll(lo, 32, 1))
        zu = jnp.where(z_pos < SIDE - 1, pltpu.roll(v, LANES - 1, 1), ghost)
        zl = jnp.where(z_pos > 0, pltpu.roll(v, 1, 1), ghost)
        return v, ((V[vp, j, plane(x + 1)] + V[vp, j, plane(x - 1)]) + (up + lo)) + (zu + zl)

    def fine_rows(j, x):
        return pl.ds(x * 8 * slots + j, 8, stride=slots)

    def edges(vp, par):
        for j in range(slots):
            V[vp, j, plane(-1)] = G[par, j, 0]
            V[vp, j, plane(SIDE)] = G[par, j, FOOT - 1]

    def fine_sweep(vp, par):
        @pl.loop(0, FOOT, unroll=4)
        def _(X):
            for j in range(slots):
                ghost = G[par, j, X]
                for e in range(2):
                    x = 2 * X + e
                    v, s = beside_fine(vp, par, j, x, ghost)
                    V[1 - vp, j, plane(x)] = KEEP * v + FW[j, x] * (FS[j, x] + s)

    shrink_lane = ((lane % 32) // FOOT) * 64 + 2 * (lane % FOOT)

    def fine_remainder(vp, par, occupied):
        def body(X, totals):
            totals = list(totals)
            for j in range(slots):
                ghost = G[par, j, X]
                for e in range(2):
                    x = 2 * X + e
                    v, s = beside_fine(vp, par, j, x, ghost)
                    r = (FS[j, x] - FD[j, x] * v) + s
                    totals[j] = totals[j] + r * r
                    V[1 - vp, j, plane(x)] = r
            return tuple(totals)

        zero = jnp.zeros(tile, jnp.float32)
        totals = lax.fori_loop(0, FOOT, body, (zero,) * slots, unroll=4)

        @pl.loop(0, FOOT // 4)
        def _(xg):
            for j in range(slots):
                acc = zero
                for k in range(4):
                    x = 2 * (xg * 4 + k)
                    t = V[1 - vp, j, plane(x)] + V[1 - vp, j, plane(x + 1)]
                    t = t + pltpu.roll(t, LANES - 1, 1)
                    t = t + pltpu.roll(t, LANES - 32, 1)
                    acc = jnp.where(lane // 32 == k, take(t, shrink_lane), acc)
                R[j, pl.ds(pl.multiple_of(xg * 8, 8), 8)] = acc * 0.125

        total = zero
        for j in range(slots):
            total = total + jnp.where(occupied[j], totals[j], 0.0)
        return total

    def pack_returns():
        for q in range(group):
            which = slotid[q]
            for g in range(4):
                rows = pl.ds(g * 8, 8)
                acc = jnp.zeros(tile, jnp.float32)
                for j in range(slots):
                    acc = jnp.where(which == float(j), R[j, rows], acc)
                rout[q, rows] = acc

    def deposit():
        @pl.loop(0, FOOT // 4)
        def _(xg):
            rows = pl.ds(pl.multiple_of(xg * 8, 8), 8)
            tiles = []
            for s in range(slots):
                tiles.append(rrec[jnp.minimum(owner[0, s], group - 1), rows])
            for k in range(4):
                x = xg * 4 + k
                for yl in range(2):
                    idx = k * 32 + yl * FOOT + lane % FOOT
                    got = []
                    for s in range(slots):
                        col = jnp.where(box_live[s], box_col[s], -1)
                        got.append(jnp.where(lane // FOOT == col, take(tiles[s], idx), 0.0))
                    for b in range(along_y):
                        place = pl.ds(b * FOOT + yl, 8, stride=2)
                        acc = c_src[x, place, :]
                        for s in range(slots):
                            acc = acc + jnp.where(box_row[s] == b, got[s], 0.0)
                        comp[x, place, :] = acc

    def halo_copies(p, which=range(6)):
        faces = (
            (U.at[p, 1], U.at[p, nx + 1]),
            (U.at[p, nx], U.at[p, 0]),
            (ys.at[0], yh.at[p, 1]),
            (ys.at[1], yh.at[p, 0]),
            (zs.at[0], zh.at[p, 1]),
            (zs.at[1], zh.at[p, 0]),
        )
        copies = []
        for i in which:
            source, target = faces[i]
            copies.append(
                pltpu.make_async_remote_copy(
                    src_ref=source,
                    dst_ref=target,
                    send_sem=h_send.at[p, i],
                    recv_sem=h_recv.at[p, i ^ 1],
                    device_id=beside[i],
                    device_id_type=MESH,
                )
            )
        return copies

    def halo_waits(p):
        places = (
            U.at[p, 0],
            U.at[p, nx + 1],
            yh.at[p, 0],
            yh.at[p, 1],
            zh.at[p, 0],
            zh.at[p, 1],
        )
        copies = []
        for i, target in enumerate(places):
            copies.append(
                pltpu.make_async_remote_copy(
                    src_ref=target,
                    dst_ref=target,
                    send_sem=h_send.at[p, i],
                    recv_sem=h_recv.at[p, i],
                    device_id=beside[i],
                    device_id_type=MESH,
                )
            )
        return copies

    def send_halos(p, which):
        for i, copy in zip(which, halo_copies(p, which)):
            pl.when(have[i])(copy.start)

    def wait_halos(p):
        for i, (sent, got) in enumerate(zip(halo_copies(p), halo_waits(p))):

            @pl.when(have[i])
            def _():
                sent.wait_send()
                got.wait_recv()

    groups = ny // 8
    per = min(groups, LANES // nx)

    def keep_y(p):
        for x in range(nx):
            ys[0, pl.ds(x, 1), :] = U[p, x + 1, pl.ds(0, 1), :]
            ys[1, pl.ds(x, 1), :] = U[p, x + 1, pl.ds(ny - 1, 1), :]

    def keep_z(p):
        for t in range(groups // per):

            def body(x, faces):
                zlo, zhi = faces
                for g in range(per):
                    at = g * nx + x
                    u = U[p, x + 1, pl.ds((t * per + g) * 8, 8)]
                    zlo = jnp.where(lane == at, pltpu.roll(u, at, 1), zlo)
                    zhi = jnp.where(lane == at, pltpu.roll(u, (at + 1) % LANES, 1), zhi)
                return zlo, zhi

            empty = jnp.zeros(tile, jnp.float32)
            zlo, zhi = lax.fori_loop(0, nx // 4, lambda i, f: body(4 * i + 3, body(4 * i + 2, body(4 * i + 1, body(4 * i, f)))), (empty, empty))
            zs[0, pl.ds(t * 8, 8)] = zlo
            zs[1, pl.ds(t * 8, 8)] = zhi

    def send_faces(p):
        send_halos(p, (0, 1))
        keep_y(p)
        send_halos(p, (2, 3))
        keep_z(p)
        send_halos(p, (4, 5))

    def z_column(packed, x, to):
        tiles = []
        for g in range(groups):
            at = (g % per) * nx + x
            face = packed[8 * (g // per) : 8 * (g // per) + 8]
            shift = (to - at) % LANES
            tiles.append(pltpu.roll(face, shift, 1) if shift else face)
        return jnp.concatenate(tiles, axis=0)

    none = jnp.zeros(wide, jnp.float32)

    def coarse_sweep(p, want_square):
        zl = zh[p, 0]
        zu = zh[p, 1]

        total = none
        for x in range(nx):
            u = U[p, x + 1]
            ym = jnp.where(wsub == 0, yh[p, 0, pl.ds(x, 1), :], pltpu.roll(u, 1, 0))
            yp = jnp.where(wsub == ny - 1, yh[p, 1, pl.ds(x, 1), :], pltpu.roll(u, ny - 1, 0))
            zm = jnp.where(wlane == 0, z_column(zl, x, 0), pltpu.roll(u, 1, 1))
            zp = jnp.where(wlane == nz - 1, z_column(zu, x, nz - 1), pltpu.roll(u, nz - 1, 1))
            s = ((U[p, x] + U[p, x + 2]) + (ym + yp)) + (zm + zp)
            s = s + comp[x]
            U[1 - p, x + 1] = KEEP * u + W[x] * s
            if want_square:
                last = s - (6.0 + c_shift[x]) * u
                total = total + last * last
        return total

    loads[0].wait()
    pack_parents(0)
    parent_copies = exchange(pout, prec, p_send, p_recv, 40)
    send_faces(0)

    for load in loads[1:]:
        load.wait()

    @pl.loop(0, nx)
    def _(x):
        W[x] = OMEGA / (6.0 + c_shift[x])

    @pl.loop(0, SIDE)
    def _(x):
        for j in range(slots):
            rows = fine_rows(j, x)
            V[0, j, plane(x)] = f_start[rows, :]
            FS[j, x] = f_src[rows, :]
            FD[j, x] = 6.0 + f_shift[rows, :]
            FW[j, x] = OMEGA / FD[j, x]

    vp = 0
    return_copies = []
    for cycle in range(CYCLES):
        par = cycle % 2
        arrive(pout, prec, p_send, p_recv, 40)
        if cycle == 0:
            count = slot_masks()
            occupied = [count > float(j) for j in range(slots)]
        ghosts(par)
        if cycle > 0:

            @pl.loop(0, FOOT)
            def _(X):
                for j in range(slots):
                    delta = G[par, j, X] - G[1 - par, j, X]
                    for e in range(2):
                        V[vp, j, plane(2 * X + e)] = V[vp, j, plane(2 * X + e)] + delta

        edges(0, par)
        edges(1, par)
        for sweep in range(FSWEEPS):
            fine_sweep(vp, par)
            vp = 1 - vp
        square = fine_remainder(vp, par, occupied)
        for copy in return_copies:
            copy.wait_send()
        pack_returns()
        return_copies = exchange(rout, rrec, r_send, r_recv, 32)
        arrive(rout, rrec, r_send, r_recv, 32)
        deposit()
        for sweep in range(CSWEEPS):
            p = sweep % 2
            final = cycle == CYCLES - 1 and sweep == CSWEEPS - 1
            wait_halos(p)
            total = coarse_sweep(p, sweep == CSWEEPS - 1)
            if not final and sweep < CSWEEPS - 1:
                send_faces(1 - p)
        for g in range(ny // 8):
            square = square + total[8 * g : 8 * g + 8]
        sums[cycle] = square
        for copy in parent_copies:
            copy.wait_send()
        pack_parents(0)
        if cycle == CYCLES - 1:
            both = jnp.where(
                sub == 0,
                jnp.sum(sums[0], axis=0, keepdims=True),
                jnp.where(sub == 1, jnp.sum(sums[1], axis=0, keepdims=True), 0.0),
            )
            for q in range(group):
                pout[q, pl.ds(32, 8)] = both
        parent_copies = exchange(pout, prec, p_send, p_recv, 40)
        if cycle < CYCLES - 1:
            send_faces(0)

    for x in range(nx):
        pot_out[x] = U[0, x + 1]

    for copy in return_copies:
        copy.wait_send()
    arrive(pout, prec, p_send, p_recv, 40)
    for copy in parent_copies:
        copy.wait_send()

    mine = jnp.zeros(tile, jnp.float32)
    for q in range(group):
        mine = mine + prec[q, pl.ds(32, 8)]
    xsum[gx] = mine
    norm_copies = []
    for d in range(1, n_gx):
        copy = pltpu.make_async_remote_copy(
            src_ref=xsum.at[gx],
            dst_ref=xsum.at[gx],
            send_sem=n_send.at[d],
            recv_sem=n_recv.at[d],
            device_id=((gx + d) % n_gx, gy, gz),
            device_id_type=MESH,
        )
        copy.start()
        norm_copies.append(copy)

    par = CYCLES % 2
    ghosts(par)

    @pl.loop(0, FOOT)
    def _(X):
        for j in range(slots):
            delta = G[par, j, X] - G[1 - par, j, X]
            for e in range(2):
                x = 2 * X + e
                fine_out[fine_rows(j, x), :] = jnp.where(occupied[j], V[vp, j, plane(x)] + delta, 0.0)

    for d in range(1, n_gx):
        source = (gx + n_gx - d) % n_gx
        pltpu.make_async_remote_copy(
            src_ref=xsum.at[source],
            dst_ref=xsum.at[source],
            send_sem=n_send.at[d],
            recv_sem=n_recv.at[d],
            device_id=(source, gy, gz),
            device_id_type=MESH,
        ).wait_recv()
    for copy in norm_copies:
        copy.wait_send()
    whole = jnp.zeros(tile, jnp.float32)
    for d in range(n_gx):
        whole = whole + xsum[d]
    cells = float(nx * ny * nz * n_gx * group)
    whole = jnp.sum(whole, axis=1, keepdims=True) / cells
    norm_out[...] = jnp.broadcast_to(jnp.sqrt(whole), tile)


def finish(norms, pot, rows, pot_out, rows_out, norm_out, sem):
    stores = [pltpu.make_async_copy(pot, pot_out, sem.at[0]), pltpu.make_async_copy(rows, rows_out, sem.at[1])]
    for store in stores:
        store.start()
    for k in range(CYCLES):
        norm_out[k] = norms[k, 0]
    for store in stores:
        store.wait()


def to_rows(a):
    slots, fine = a.shape
    return a.reshape(slots, fine // LANES, LANES).transpose(1, 0, 2).reshape(slots * fine // LANES, LANES)


def from_rows(a, slots):
    return a.reshape(-1, slots, LANES).transpose(1, 0, 2).reshape(slots, -1)


def local(sizes, c_src, c_shift, c_start, f_src, f_shift, f_start, corner, owner):
    n_gx, n_gy, n_gz = sizes
    group = n_gy * n_gz
    slots = owner.shape[1]
    nx, ny, nz = c_src.shape
    fine = f_src.shape[1]
    f32 = jnp.float32
    face_rows = ny // min(ny // 8, LANES // nx)
    vmem = pl.BlockSpec(memory_space=pltpu.VMEM)
    smem = pl.BlockSpec(memory_space=pltpu.SMEM)
    dma = pltpu.SemaphoreType.DMA
    pot, rows, norms = pl.pallas_call(
        functools.partial(kernel, sizes),
        out_shape=(
            pltpu.VMEM((nx, ny, nz), f32),
            pltpu.VMEM((slots * fine // LANES, LANES), f32),
            pltpu.VMEM((8, LANES), f32),
        ),
        in_specs=[smem, smem] + [pl.BlockSpec(memory_space=pl.ANY)] * 6,
        out_specs=(vmem, vmem, vmem),
        scratch_shapes=[
            pltpu.VMEM((nx, ny, nz), f32),
            pltpu.VMEM((nx, ny, nz), f32),
            pltpu.VMEM((slots * fine // LANES, LANES), f32),
            pltpu.VMEM((slots * fine // LANES, LANES), f32),
            pltpu.VMEM((slots * fine // LANES, LANES), f32),
            dma((6,)),
            pltpu.VMEM((2, nx + 2, ny, nz), f32),
            pltpu.VMEM((nx, ny, nz), f32),
            pltpu.VMEM((nx, ny, nz), f32),
            pltpu.VMEM((2, 2, nx, nz), f32),
            pltpu.VMEM((2, nx, nz), f32),
            pltpu.VMEM((2, 2, face_rows, nz), f32),
            pltpu.VMEM((2, face_rows, nz), f32),
            pltpu.VMEM((2, slots, (SIDE + 2) * 8, LANES), f32),
            pltpu.VMEM((slots, SIDE, 8, LANES), f32),
            pltpu.VMEM((slots, SIDE, 8, LANES), f32),
            pltpu.VMEM((slots, SIDE, 8, LANES), f32),
            pltpu.VMEM((2, slots, FOOT, 8, LANES), f32),
            pltpu.VMEM((slots, 32, LANES), f32),
            pltpu.VMEM((slots, 32, LANES), f32),
            pltpu.VMEM((group, 40, LANES), f32),
            pltpu.VMEM((group, 40, LANES), f32),
            pltpu.VMEM((group, 32, LANES), f32),
            pltpu.VMEM((group, 32, LANES), f32),
            pltpu.VMEM((group, 8, LANES), f32),
            pltpu.VMEM((CYCLES, 8, LANES), f32),
            pltpu.VMEM((n_gx, 8, LANES), f32),
            dma((group,)),
            dma((group,)),
            dma((group,)),
            dma((group,)),
            dma((2, 6)),
            dma((2, 6)),
            dma((n_gx,)),
            dma((n_gx,)),
        ],
        compiler_params=pltpu.CompilerParams(collective_id=0, has_side_effects=True, vmem_limit_bytes=63000000),
    )(corner.transpose(2, 0, 1), owner, c_src, c_shift, c_start, to_rows(f_src), to_rows(f_shift), to_rows(f_start))
    anywhere = pl.BlockSpec(memory_space=pl.ANY)
    pot, rows, norms = pl.pallas_call(
        finish,
        out_shape=(
            jax.ShapeDtypeStruct(pot.shape, f32),
            jax.ShapeDtypeStruct(rows.shape, f32),
            jax.ShapeDtypeStruct((CYCLES,), f32),
        ),
        in_specs=[smem, vmem, vmem],
        out_specs=(anywhere, anywhere, smem),
        scratch_shapes=[dma((2,))],
        compiler_params=pltpu.CompilerParams(vmem_limit_bytes=8 << 20),
    )(norms, pot, rows)
    return pot, from_rows(rows, slots), norms


def solution(mesh):
    sizes = (mesh.shape["gx"], mesh.shape["gy"], mesh.shape["gz"])
    everywhere = ("gx", "gy", "gz")
    block = P(*everywhere)
    in_specs = (
        block,
        block,
        block,
        P(everywhere, None),
        P(everywhere, None),
        P(everywhere, None),
        P(everywhere, None, None),
        P(everywhere, None),
    )
    out_specs = (block, P(everywhere, None), P())
    return jax.shard_map(
        functools.partial(local, sizes), mesh=mesh, in_specs=in_specs, out_specs=out_specs, check_vma=False
    )
```

```python
import functools
import itertools

import jax
import jax.numpy as jnp
from jax import lax
from jax.experimental import pallas as pl
from jax.experimental.pallas import tpu as pltpu
from jax.sharding import PartitionSpec as P

FOOT = 16
CYCLES = 2
CSWEEPS = 4
FSWEEPS = 3
OMEGA = 0.8
KEEP = 1.0 - OMEGA
MESH = pl.DeviceIdType.MESH
LANES = 128
SIDE = 2 * FOOT
DEEP = CSWEEPS
PAD = 8
DIRS = [d for d in itertools.product((-1, 0, 1), repeat=3) if any(d)]
FPLANE = SIDE + 8


def take(x, idx):
    return jnp.take_along_axis(x, idx, axis=1, mode="promise_in_bounds")


def iota(shape, dim):
    return lax.broadcasted_iota(jnp.int32, shape, dim)


def turn(x, by):
    by = by % LANES
    return pltpu.roll(x, by, 1) if by else x


def kernel(
    sizes,
    corner,
    owner,
    c_src_hbm,
    c_shift_hbm,
    c_start_hbm,
    f_src_hbm,
    f_shift_hbm,
    f_start_hbm,
    pot_out,
    fine_out,
    norm_out,
    c_shift,
    f_src,
    f_shift,
    f_start,
    in_sem,
    P0,
    P1,
    W0,
    W1,
    C0,
    C1,
    E0,
    A0,
    A1,
    B0,
    B1,
    Q0,
    Q1,
    pk,
    zs,
    V0,
    V1,
    T,
    FW,
    FS,
    FD,
    G,
    PRE,
    compact,
    R,
    pout,
    prec,
    rout,
    rrec,
    slotid,
    sums,
    xsum,
    gsum,
    p_send,
    p_recv,
    r_send,
    r_recv,
    h_send,
    h_recv,
    n_send,
    n_recv,
    g_send,
    g_recv,
):
    n_gx, n_gy, n_gz = sizes
    group = n_gy * n_gz
    slots = owner.shape[1]
    nx, ny, nz = c_src_hbm.shape
    along_y = ny // FOOT
    first, rows = PAD + 8, ny + 16
    inner, block = pl.ds(first, ny), pl.ds(PAD, rows)
    inside = pl.ds(DEEP, nx)
    gx, gy, gz = lax.axis_index("gx"), lax.axis_index("gy"), lax.axis_index("gz")
    me = gy * n_gz + gz
    V = (V0, V1)
    zero_rows = jnp.zeros((rows, LANES), jnp.float32)
    zero_tile = jnp.zeros((8, LANES), jnp.float32)

    def rank_id(rank):
        return (gx, rank // n_gz, rank % n_gz)

    loads = [
        pltpu.make_async_copy(source, target, in_sem.at[i])
        for i, (source, target) in enumerate(
            (
                (c_start_hbm, P0.at[inside, inner]),
                (c_shift_hbm, c_shift),
                (c_src_hbm, C0.at[inside, inner]),
                (f_start_hbm, f_start),
                (f_src_hbm, f_src),
                (f_shift_hbm, f_shift),
            )
        )
    ]
    for load in loads:
        load.start()

    for F in (P0, W0, C0, E0):
        for X in range(nx + 2 * DEEP):
            if DEEP <= X < DEEP + nx:
                F[X, pl.ds(PAD, 8)] = zero_tile
                F[X, pl.ds(first + ny, 8)] = zero_tile
            else:
                F[X, block] = zero_rows
    for f in range(4):
        for a in range(3):
            for b in range(2):
                zs[f, a, b] = zero_rows

    barrier = pltpu.get_barrier_semaphore()
    greeted = group - 1 + n_gx - 1
    for d in range(1, group):
        pl.semaphore_signal(barrier, inc=1, device_id=rank_id((me + d) % group), device_id_type=MESH)
    for d in range(1, n_gx):
        pl.semaphore_signal(barrier, inc=1, device_id=((gx + d) % n_gx, gy, gz), device_id_type=MESH)
    for dx, dy, dz in DIRS:
        if dx and (dy or dz):
            other = ((gx + dx + n_gx) % n_gx, (gy + dy + n_gy) % n_gy, (gz + dz + n_gz) % n_gz)
            pl.semaphore_signal(barrier, inc=1, device_id=other, device_id_type=MESH)
            greeted += 1

    tile = (8, LANES)
    lane = iota(tile, 1)
    part = lane // SIDE
    box_row = []
    box_col = []
    box_live = []
    for s in range(slots):
        box_row.append((corner[1, 0, s] // 2 - gy * ny) // FOOT)
        box_col.append((corner[2, 0, s] // 2 - gz * nz) // FOOT)
        box_live.append(owner[0, s] < group)

    def exchange(out, rec, send, recv, count):
        copies = []
        for d in range(1, group):
            peer = (me + d) % group
            copy = pltpu.make_async_remote_copy(
                src_ref=out.at[peer, pl.ds(0, count)],
                dst_ref=rec.at[me, pl.ds(0, count)],
                send_sem=send.at[d],
                recv_sem=recv.at[d],
                device_id=rank_id(peer),
                device_id_type=MESH,
            )
            copy.start()
            copies.append(copy)
        rec[me, pl.ds(0, count)] = out[me, pl.ds(0, count)]
        return copies

    def arrive(out, rec, send, recv, count):
        for d in range(1, group):
            source = (me + group - d) % group
            pltpu.make_async_remote_copy(
                src_ref=out.at[source, pl.ds(0, count)],
                dst_ref=rec.at[source, pl.ds(0, count)],
                send_sem=send.at[d],
                recv_sem=recv.at[d],
                device_id=rank_id(source),
                device_id_type=MESH,
            ).wait_recv()

    def pack_parents():
        for m in range(FOOT // 4):
            for s in range(slots):
                idx = box_col[s] * FOOT + (lane % FOOT)
                acc = jnp.zeros(tile, jnp.float32)
                for k in range(4):
                    for h in range(2):
                        X = DEEP + 4 * m + k
                        a = P0[X, pl.ds(first + 8 * h, 8)]
                        for b in range(1, along_y):
                            other = P0[X, pl.ds(first + FOOT * b + 8 * h, 8)]
                            a = jnp.where(box_row[s] == b, other, a)
                        acc = jnp.where(lane // FOOT == 2 * k + h, take(a, idx), acc)
                compact[s, pl.ds(8 * m, 8), :] = acc

        for q in range(group):
            acc = jnp.zeros((32, LANES), jnp.float32)
            for s in range(slots):
                acc = jnp.where(owner[0, s] == q, compact[s], acc)
            pout[q, pl.ds(0, 32)] = acc

    def pack_flags():
        for q in range(group):
            flag = zero_tile
            for s in range(slots):
                flag = jnp.where(owner[0, s] == q, 1.0, flag)
            pout[q, pl.ds(32, 8)] = flag

    def slot_masks():
        count = zero_tile
        for q in range(group):
            flag = prec[q, pl.ds(32, 8)]
            slotid[q] = jnp.where(flag > 0.5, count, -1.0)
            count = count + flag
        return count

    def ghosts(par):
        for m in range(FOOT // 4):
            at = pl.ds(8 * m, 8)
            tiles = []
            for j in range(slots):
                acc = zero_tile
                for q in range(group):
                    acc = jnp.where(slotid[q] == float(j), prec[q, at], acc)
                tiles.append(acc)
            for k in range(4):
                for h in range(2):
                    idx = k * 32 + h * FOOT + (lane % SIDE) // 2
                    acc = take(tiles[0], idx)
                    for j in range(1, slots):
                        acc = jnp.where(part == j, take(tiles[j], idx), acc)
                    for e in range(2):
                        G[par, 4 * m + k, pl.ds(2 * 8 * h + e, 8, stride=2), :] = acc

    wide = (SIDE, LANES)
    z_pos = iota(wide, 1) % SIDE

    def start_of(x):
        return 8 + (x + 1) * FPLANE

    def edges(par):
        for v in V:
            v[pl.ds(start_of(-1), SIDE)] = G[par, 0]
            v[pl.ds(start_of(SIDE), SIDE)] = G[par, FOOT - 1]
            for X in range(FOOT):
                low = G[par, X, pl.ds(0, 1)]
                top = G[par, X, pl.ds(SIDE - 1, 1)]
                for e in range(2):
                    v[pl.ds(start_of(2 * X + e) - 1, 1)] = low
                    v[pl.ds(start_of(2 * X + e) + SIDE, 1)] = top

    def beside_fine(v, par, x):
        at = start_of(x)
        u = v[pl.ds(at, SIDE)]
        ghost = G[par, x // 2]
        zu = jnp.where(z_pos < SIDE - 1, turn(u, -1), ghost)
        zl = jnp.where(z_pos > 0, turn(u, 1), ghost)
        across = v[pl.ds(at + FPLANE, SIDE)] + v[pl.ds(at - FPLANE, SIDE)]
        along = v[pl.ds(at + 1, SIDE)] + v[pl.ds(at - 1, SIDE)]
        return u, (across + along) + (zu + zl)

    def fine_sweep(vp, par):
        for x in range(SIDE):
            u, s = beside_fine(V[vp], par, x)
            V[1 - vp][pl.ds(start_of(x), SIDE)] = KEEP * u + FW[x] * (FS[x] + s)

    def fine_remainder(vp, par):
        total = jnp.zeros(wide, jnp.float32)
        for X in range(FOOT):
            t = None
            for e in range(2):
                x = 2 * X + e
                u, s = beside_fine(V[vp], par, x)
                r = (FS[x] - FD[x] * u) + s
                total = total + r * r
                t = r if t is None else t + r
            T[X] = t + turn(t, -1)
        square = zero_tile
        for g in range(SIDE // 8):
            square = square + total[8 * g : 8 * g + 8]
        return square

    def shrink():
        for m in range(FOOT // 4):
            packed = []
            for k in range(4):
                X = 4 * m + k
                halves = []
                for h in range(2):
                    even = T[X, pl.ds(16 * h, 8, stride=2), :]
                    odd = T[X, pl.ds(16 * h + 1, 8, stride=2), :]
                    halves.append(even + odd)
                packed.append(jnp.where(lane % 2 == 0, halves[0], turn(halves[1], 1)) * 0.125)
            for j in range(slots):
                acc = turn(packed[0], -SIDE * j)
                for k in range(1, 4):
                    acc = jnp.where(part == k, turn(packed[k], SIDE * (k - j)), acc)
                R[j, pl.ds(8 * m, 8)] = acc

    def pack_returns():
        for q in range(group):
            which = slotid[q]
            for m in range(FOOT // 4):
                at = pl.ds(m * 8, 8)
                acc = zero_tile
                for j in range(slots):
                    acc = jnp.where(which == float(j), R[j, at], acc)
                rout[q, at] = acc

    def deposit():
        for m in range(FOOT // 4):
            tiles = []
            for s in range(slots):
                tiles.append(rrec[jnp.minimum(owner[0, s], group - 1), pl.ds(8 * m, 8)])
            for k in range(4):
                X = DEEP + 4 * m + k
                for h in range(2):
                    idx = k * 32 + (lane % FOOT) * 2 + h
                    got = []
                    for s in range(slots):
                        col = jnp.where(box_live[s], box_col[s], -1)
                        got.append(jnp.where(lane // FOOT == col, take(tiles[s], idx), 0.0))
                    for b in range(along_y):
                        acc = jnp.where(box_row[0] == b, got[0], 0.0)
                        for s in range(1, slots):
                            acc = acc + jnp.where(box_row[s] == b, got[s], 0.0)
                        E0[X, pl.ds(first + FOOT * b + 8 * h, 8)] = acc

    tall = iota((ny, LANES), 1)

    def pack_lanes(F, f):
        acc = turn(F[DEEP, inner], DEEP)
        for x in range(1, nx):
            acc = jnp.where(tall // (2 * DEEP) == x, turn(F[DEEP + x, inner], 2 * DEEP * x + DEEP), acc)
        pk[f] = acc

    def regions(F, f, depth, d):
        dx, dy, dz = d
        x_src = {0: inside, -1: pl.ds(DEEP, depth), 1: pl.ds(DEEP + nx - depth, depth)}[dx]
        x_dst = {0: inside, -1: pl.ds(DEEP + nx, depth), 1: pl.ds(DEEP - depth, depth)}[dx]
        if dz == 0:
            y_src = {0: inner, -1: pl.ds(first, 8), 1: pl.ds(first + ny - 8, 8)}[dy]
            y_dst = {0: inner, -1: pl.ds(first + ny, 8), 1: pl.ds(PAD, 8)}[dy]
            return F.at[x_src, y_src], F.at[x_dst, y_dst]
        y_src = {0: pl.ds(0, ny), -1: pl.ds(0, 8), 1: pl.ds(ny - 8, 8)}[dy]
        y_dst = {0: pl.ds(8, ny), -1: pl.ds(8 + ny, 8), 1: pl.ds(0, 8)}[dy]
        return pk.at[f, y_src], zs.at[f, {0: 0, -1: 1, 1: 2}[dx], 0 if dz < 0 else 1, y_dst]

    def there(d):
        tests = []
        for step, at, count in zip(d, (gx, gy, gz), sizes):
            if step < 0:
                tests.append(at > 0)
            if step > 0:
                tests.append(at < count - 1)
        return functools.reduce(jnp.logical_and, tests)

    def halo_copy(F, f, depth, i):
        d = DIRS[i]
        source, target = regions(F, f, depth, d)
        return pltpu.make_async_remote_copy(
            src_ref=source,
            dst_ref=target,
            send_sem=h_send.at[f, i],
            recv_sem=h_recv.at[f, len(DIRS) - 1 - i],
            device_id=(gx + d[0], gy + d[1], gz + d[2]),
            device_id_type=MESH,
        )

    def halo_wait(F, f, depth, i):
        d = DIRS[i]
        _, target = regions(F, f, depth, tuple(-v for v in d))
        return pltpu.make_async_remote_copy(
            src_ref=target,
            dst_ref=target,
            send_sem=h_send.at[f, i],
            recv_sem=h_recv.at[f, i],
            device_id=(gx + d[0], gy + d[1], gz + d[2]),
            device_id_type=MESH,
        )

    far_first = sorted(range(len(DIRS)), key=lambda i: -sum(map(abs, DIRS[i])))

    def send_halo(F, f, depth):
        pack_lanes(F, f)
        for i in far_first:
            pl.when(there(DIRS[i]))(halo_copy(F, f, depth, i).start)

    def wait_halo(F, f, depth):
        for i in reversed(far_first):

            @pl.when(there(DIRS[i]))
            def _():
                halo_copy(F, f, depth, i).wait_send()
                halo_wait(F, f, depth, i).wait_recv()

    low_part = iota((rows, LANES), 1) % (2 * DEEP) >= DEEP

    def lane_halo(f, depth):
        merged = [jnp.where(low_part, zs[f, a, 0], zs[f, a, 1]) for a in range(3)]
        for X in range(DEEP - depth, DEEP + nx + depth):
            if X < DEEP:
                a, i = 2, nx - DEEP + X
            elif X < DEEP + nx:
                a, i = 0, X - DEEP
            else:
                a, i = 1, X - DEEP - nx
            yield X, turn(merged[a], -(2 * DEEP * i + DEEP))

    def unpack_lanes(f, F1):
        for X, value in lane_halo(f, DEEP):
            F1[X, block] = value

    def sweep(source, target, comp, depth, squares=False):
        U0, U1 = source
        count = rows if depth else ny
        off = PAD if depth else first
        here, up, down = pl.ds(off, count), pl.ds(off + 1, count), pl.ds(off - 1, count)
        wlane = iota((count, LANES), 1)
        left, right = wlane == 0, wlane == LANES - 1
        total = jnp.zeros((count, LANES), jnp.float32)
        for X in range(DEEP - depth, DEEP + nx + depth):
            u = (U0[X, here], U1[X, here])
            prev = [turn(v, 1) for v in u]
            nxt = [turn(v, -1) for v in u]
            for t in range(2 if depth else 1):
                U = source[t]
                z = jnp.where(left, prev[1 - t], prev[t]) + jnp.where(right, nxt[1 - t], nxt[t])
                s = ((U[X - 1, here] + U[X + 1, here]) + (U[X, up] + U[X, down])) + z
                s = s + comp[t][X, here]
                target[t][X, here] = KEEP * u[t] + (W0, W1)[t][X, here] * s
                if squares:
                    last = s - (6.0 + c_shift[X - DEEP]) * u[t]
                    total = total + last * last
        return total

    def add_deposit(X, at, t, e):
        A, W, C, Q = ((A0, W0, C0, Q0), (A1, W1, C1, Q1))[t]
        A[X, at] = A[X, at] + W[X, at] * e
        Q[X, at] = C[X, at] + e

    loads[0].wait()
    pack_parents()
    pack_flags()
    loads[1].wait()
    for x in range(nx):
        W0[DEEP + x, inner] = OMEGA / (6.0 + c_shift[x])
    pl.semaphore_wait(barrier, greeted)
    parent_copies = exchange(pout, prec, p_send, p_recv, 40)
    send_halo(P0, 0, DEEP)
    send_halo(W0, 1, DEEP - 1)
    loads[2].wait()
    send_halo(C0, 2, DEEP - 1)

    for load in loads[3:]:
        load.wait()

    def spread(a, x):
        parts = [a[pl.ds(x * 8 * slots + j, 8, stride=slots), :] for j in range(slots)]
        result = []
        for w in range(SIDE // 8):
            acc = turn(parts[0], -SIDE * w)
            for j in range(1, slots):
                acc = jnp.where(part == j, turn(parts[j], SIDE * (j - w)), acc)
            result.append(acc)
        return result

    def gather(parts):
        result = []
        for j in range(slots):
            acc = turn(parts[0], -SIDE * j)
            for w in range(1, SIDE // 8):
                acc = jnp.where(part == w, turn(parts[w], SIDE * (w - j)), acc)
            result.append(acc)
        return result

    def prepare():
        @pl.loop(0, SIDE, unroll=4)
        def _(x):
            for w, value in enumerate(spread(f_start, x)):
                V0[pl.ds(8 + (x + 1) * FPLANE + w, 8, stride=4), :] = value
            for w, value in enumerate(spread(f_src, x)):
                FS[x, pl.ds(w, 8, stride=4), :] = value
            for w, value in enumerate(spread(f_shift, x)):
                diagonal = 6.0 + value
                FD[x, pl.ds(w, 8, stride=4), :] = diagonal
                FW[x, pl.ds(w, 8, stride=4), :] = OMEGA / diagonal

    prepare()

    vp = 0
    return_copies = []
    for cycle in range(CYCLES):
        par = cycle % 2
        arrive(pout, prec, p_send, p_recv, 32 if cycle else 40)
        if cycle == 0:
            count = slot_masks()
            occupied = [count > float(j) for j in range(slots)]
            live_lanes = count > part.astype(jnp.float32)
        ghosts(par)
        if cycle > 0:
            for x in range(SIDE):
                at = pl.ds(start_of(x), SIDE)
                V[vp][at] = V[vp][at] + (G[par, x // 2] - G[1 - par, x // 2])
        edges(par)
        for _ in range(FSWEEPS):
            fine_sweep(vp, par)
            vp = 1 - vp
        square = jnp.where(live_lanes, fine_remainder(vp, par), 0.0)
        shrink()
        for copy in return_copies:
            copy.wait_send()
        pack_returns()
        return_copies = exchange(rout, rrec, r_send, r_recv, 32)
        wait_halo(P0, 0, DEEP)
        unpack_lanes(0, P1)
        if cycle == 0:
            wait_halo(W0, 1, DEEP - 1)
            unpack_lanes(1, W1)
            wait_halo(C0, 2, DEEP - 1)
            unpack_lanes(2, C1)
        sweep((P0, P1), (A0, A1), (C0, C1), DEEP - 1)
        arrive(rout, rrec, r_send, r_recv, 32)
        deposit()
        send_halo(E0, 3, DEEP - 1)
        for x in range(nx):
            add_deposit(DEEP + x, inner, 0, E0[DEEP + x, inner])
        wait_halo(E0, 3, DEEP - 1)
        for X in range(1, nx + 2 * DEEP - 1):
            if DEEP <= X < DEEP + nx:
                for at in (pl.ds(PAD, 8), pl.ds(first + ny, 8)):
                    add_deposit(X, at, 0, E0[X, at])
            else:
                add_deposit(X, block, 0, E0[X, block])
        for X, value in lane_halo(3, DEEP - 1):
            add_deposit(X, block, 1, value)
        now, later = (A0, A1), (B0, B1)
        for depth in range(CSWEEPS - 2, 0, -1):
            sweep(now, later, (Q0, Q1), depth)
            now, later = later, now
        total = sweep(now, (P0, None), (Q0, None), 0, True)
        for g in range(ny // 8):
            square = square + total[8 * g : 8 * g + 8]
        sums[cycle] = square
        for copy in parent_copies:
            copy.wait_send()
        if cycle == CYCLES - 1:
            xsum[gx] = jnp.where(
                iota(tile, 0) == 0,
                jnp.sum(sums[0], axis=0, keepdims=True),
                jnp.where(iota(tile, 0) == 1, jnp.sum(sums[1], axis=0, keepdims=True), 0.0),
            )
            norm_copies = []
            for d in range(1, n_gx):
                copy = pltpu.make_async_remote_copy(
                    src_ref=xsum.at[gx],
                    dst_ref=xsum.at[gx],
                    send_sem=n_send.at[d],
                    recv_sem=n_recv.at[d],
                    device_id=((gx + d) % n_gx, gy, gz),
                    device_id_type=MESH,
                )
                copy.start()
                norm_copies.append(copy)
        pack_parents()
        parent_copies = exchange(pout, prec, p_send, p_recv, 32)
        if cycle < CYCLES - 1:
            send_halo(P0, 0, DEEP)

    par = CYCLES % 2
    for x in range(nx):
        pot_out[x] = P0[DEEP + x, inner]

    def settle():
        @pl.loop(0, FOOT, unroll=4)
        def _(X):
            for e in range(2):
                x = 2 * X + e
                parts = []
                for w in range(SIDE // 8):
                    old = G[1 - par, X, pl.ds(w, 8, stride=4), :]
                    parts.append(V[vp][pl.ds(8 + (x + 1) * FPLANE + w, 8, stride=4), :] - old)
                for j, value in enumerate(gather(parts)):
                    PRE[x, j] = value

    settle()
    for d in range(1, n_gx):
        source = (gx + n_gx - d) % n_gx
        pltpu.make_async_remote_copy(
            src_ref=xsum.at[source],
            dst_ref=xsum.at[source],
            send_sem=n_send.at[d],
            recv_sem=n_recv.at[d],
            device_id=(source, gy, gz),
            device_id_type=MESH,
        ).wait_recv()
    for copy in norm_copies:
        copy.wait_send()
    mine = zero_tile
    for d in range(n_gx):
        mine = mine + xsum[d]
    gsum[me] = mine
    group_copies = []
    for d in range(1, group):
        copy = pltpu.make_async_remote_copy(
            src_ref=gsum.at[me],
            dst_ref=gsum.at[me],
            send_sem=g_send.at[d],
            recv_sem=g_recv.at[d],
            device_id=rank_id((me + d) % group),
            device_id_type=MESH,
        )
        copy.start()
        group_copies.append(copy)

    for copy in return_copies:
        copy.wait_send()
    arrive(pout, prec, p_send, p_recv, 32)
    for copy in parent_copies:
        copy.wait_send()
    ghosts(par)

    def deliver():
        @pl.loop(0, FOOT, unroll=4)
        def _(X):
            parts = [G[par, X, pl.ds(w, 8, stride=4), :] for w in range(SIDE // 8)]
            for j, value in enumerate(gather(parts)):
                for e in range(2):
                    x = 2 * X + e
                    place = pl.ds(x * 8 * slots + j, 8, stride=slots)
                    fine_out[place, :] = jnp.where(occupied[j], PRE[x, j] + value, 0.0)

    deliver()
    for d in range(1, group):
        source = (me + group - d) % group
        pltpu.make_async_remote_copy(
            src_ref=gsum.at[source],
            dst_ref=gsum.at[source],
            send_sem=g_send.at[d],
            recv_sem=g_recv.at[d],
            device_id=rank_id(source),
            device_id_type=MESH,
        ).wait_recv()
    for copy in group_copies:
        copy.wait_send()
    whole = zero_tile
    for q in range(group):
        whole = whole + gsum[q]
    cells = float(nx * ny * nz * n_gx * group)
    whole = jnp.sum(whole, axis=1, keepdims=True) / cells
    norm_out[...] = jnp.broadcast_to(jnp.sqrt(whole), tile)


def finish(norms, pot, rows, pot_out, rows_out, norm_out, sem):
    stores = [pltpu.make_async_copy(pot, pot_out, sem.at[0]), pltpu.make_async_copy(rows, rows_out, sem.at[1])]
    for store in stores:
        store.start()
    for k in range(CYCLES):
        norm_out[k] = norms[k, 0]
    for store in stores:
        store.wait()


def to_rows(a):
    slots, fine = a.shape
    return a.reshape(slots, fine // LANES, LANES).transpose(1, 0, 2).reshape(slots * fine // LANES, LANES)


def from_rows(a, slots):
    return a.reshape(-1, slots, LANES).transpose(1, 0, 2).reshape(slots, -1)


def local(sizes, c_src, c_shift, c_start, f_src, f_shift, f_start, corner, owner):
    n_gx, n_gy, n_gz = sizes
    group = n_gy * n_gz
    slots = owner.shape[1]
    nx, ny, nz = c_src.shape
    fine = f_src.shape[1]
    f32 = jnp.float32
    assert 2 * DEEP * nx == LANES == nz and slots * SIDE == LANES and nx == FOOT
    vmem = pl.BlockSpec(memory_space=pltpu.VMEM)
    smem = pl.BlockSpec(memory_space=pltpu.SMEM)
    anywhere = pl.BlockSpec(memory_space=pl.ANY)
    dma = pltpu.SemaphoreType.DMA
    rows = pltpu.VMEM((slots * fine // LANES, LANES), f32)
    ring = pltpu.VMEM((nx + 2 * DEEP, ny + 5 * 8, LANES), f32)
    box = pltpu.VMEM((8 + (SIDE + 2) * FPLANE + 8, LANES), f32)
    planes = pltpu.VMEM((SIDE, SIDE, LANES), f32)
    pot, fine_rows, norms = pl.pallas_call(
        functools.partial(kernel, sizes),
        out_shape=(pltpu.VMEM((nx, ny, nz), f32), rows, pltpu.VMEM((8, LANES), f32)),
        in_specs=[smem, smem] + [anywhere] * 6,
        out_specs=(vmem, vmem, vmem),
        scratch_shapes=[pltpu.VMEM((nx, ny, nz), f32), rows, rows, rows, dma((6,))]
        + [ring] * 13
        + [
            pltpu.VMEM((4, ny, LANES), f32),
            pltpu.VMEM((4, 3, 2, ny + 16, LANES), f32),
            box,
            box,
            pltpu.VMEM((FOOT, SIDE, LANES), f32),
            planes,
            planes,
            planes,
            pltpu.VMEM((2, FOOT, SIDE, LANES), f32),
            pltpu.VMEM((SIDE, slots, 8, LANES), f32),
            pltpu.VMEM((slots, 32, LANES), f32),
            pltpu.VMEM((slots, 32, LANES), f32),
            pltpu.VMEM((group, 40, LANES), f32),
            pltpu.VMEM((group, 40, LANES), f32),
            pltpu.VMEM((group, 32, LANES), f32),
            pltpu.VMEM((group, 32, LANES), f32),
            pltpu.VMEM((group, 8, LANES), f32),
            pltpu.VMEM((CYCLES, 8, LANES), f32),
            pltpu.VMEM((n_gx, 8, LANES), f32),
            pltpu.VMEM((group, 8, LANES), f32),
            dma((group,)),
            dma((group,)),
            dma((group,)),
            dma((group,)),
            dma((4, len(DIRS))),
            dma((4, len(DIRS))),
            dma((n_gx,)),
            dma((n_gx,)),
            dma((group,)),
            dma((group,)),
        ],
        compiler_params=pltpu.CompilerParams(collective_id=0, has_side_effects=True, vmem_limit_bytes=63000000),
    )(corner.transpose(2, 0, 1), owner, c_src, c_shift, c_start, to_rows(f_src), to_rows(f_shift), to_rows(f_start))
    pot, fine_rows, norms = pl.pallas_call(
        finish,
        out_shape=(
            jax.ShapeDtypeStruct(pot.shape, f32),
            jax.ShapeDtypeStruct(fine_rows.shape, f32),
            jax.ShapeDtypeStruct((CYCLES,), f32),
        ),
        in_specs=[smem, vmem, vmem],
        out_specs=(anywhere, anywhere, smem),
        scratch_shapes=[dma((2,))],
        compiler_params=pltpu.CompilerParams(vmem_limit_bytes=8 << 20),
    )(norms, pot, fine_rows)
    return pot, from_rows(fine_rows, slots), norms


def solution(mesh):
    sizes = (mesh.shape["gx"], mesh.shape["gy"], mesh.shape["gz"])
    everywhere = ("gx", "gy", "gz")
    block = P(*everywhere)
    in_specs = (
        block,
        block,
        block,
        P(everywhere, None),
        P(everywhere, None),
        P(everywhere, None),
        P(everywhere, None, None),
        P(everywhere, None),
    )
    out_specs = (block, P(everywhere, None), P())
    return jax.shard_map(
        functools.partial(local, sizes), mesh=mesh, in_specs=in_specs, out_specs=out_specs, check_vma=False
    )
```

```python
import functools
import itertools
import math

import jax
import jax.numpy as jnp
from jax import lax
from jax.experimental import pallas as pl
from jax.experimental.pallas import tpu as pltpu
from jax.sharding import PartitionSpec as P

FOOT = 16
CYCLES = 2
CSWEEPS = 4
FSWEEPS = 3
OMEGA = 0.8
KEEP = 1.0 - OMEGA
MESH = pl.DeviceIdType.MESH
LANES = 128
SIDE = 2 * FOOT
DEEP = CSWEEPS
PAD = 8
CH = 16
PIECES = 2
FCH = 16
DIRS = [d for d in itertools.product((-1, 0, 1), repeat=3) if any(d)]
FPLANE = SIDE + 8


def take(x, idx):
    return jnp.take_along_axis(x, idx, axis=1, mode="promise_in_bounds")


def iota(shape, dim):
    return lax.broadcasted_iota(jnp.int32, shape, dim)


def turn(x, by):
    by = by % LANES
    return pltpu.roll(x, by, 1) if by else x


def kernel(
    sizes,
    corner_hbm,
    owner_hbm,
    c_src_hbm,
    c_shift_hbm,
    c_start_hbm,
    f_src_hbm,
    f_shift_hbm,
    f_start_hbm,
    pot_out,
    fine_out,
    norm_out,
    corner,
    owner,
    c_src,
    c_shift,
    f_src,
    f_shift,
    f_start,
    in_sem,
    H0,
    P1,
    W1,
    A0,
    A1,
    B0,
    B1,
    Q1,
    pk,
    zs,
    V0,
    V1,
    T,
    FW,
    FS,
    FD,
    G,
    PRE,
    compact,
    R,
    pout,
    prec,
    rout,
    rrec,
    slotid,
    sums,
    own,
    team,
    xsum,
    gsum,
    p_sem,
    r_sem,
    h_send,
    h_recv,
    n_sem,
    g_sem,
):
    n_gx, n_gy, n_gz = sizes
    group = n_gy * n_gz
    devices = n_gx * group
    direct = devices <= 64
    slots = owner_hbm.shape[1]
    nx, ny, nz = c_src_hbm.shape
    along_y = ny // FOOT
    first, rows = PAD + 8, ny + 16
    inner, block = pl.ds(first, ny), pl.ds(PAD, rows)
    inside = pl.ds(DEEP, nx)
    gx, gy, gz = lax.axis_index("gx"), lax.axis_index("gy"), lax.axis_index("gz")
    me = gy * n_gz + gz
    V = (V0, V1)
    P0, W0, E0 = (H0.at[f] for f in range(3))
    zero_rows = jnp.zeros((rows, LANES), jnp.float32)
    zero_tile = jnp.zeros((8, LANES), jnp.float32)

    def rank_id(rank):
        return (gx, rank // n_gz, rank % n_gz)

    loads = [
        pltpu.make_async_copy(source, target, in_sem.at[i])
        for i, (source, target) in enumerate(
            (
                (c_start_hbm, H0.at[0, inside, inner]),
                (c_shift_hbm, c_shift),
                (c_src_hbm, c_src),
                (f_start_hbm, f_start),
                (f_src_hbm, f_src),
                (f_shift_hbm, f_shift),
                (corner_hbm, corner),
                (owner_hbm, owner),
            )
        )
    ]
    for load in (loads[0], loads[6], loads[7]):
        load.start()

    barrier = pltpu.get_barrier_semaphore()
    greeted = 0
    for a, b, c in itertools.product(range(n_gx), range(n_gy), range(n_gz)):
        near = [min(v, n - v) for v, n in zip((a, b, c), sizes)]
        if any(near) and (direct or a == 0 or (b == 0 and c == 0) or max(near) == 1):
            other = ((gx + a) % n_gx, (gy + b) % n_gy, (gz + c) % n_gz)
            pl.semaphore_signal(barrier, inc=1, device_id=other, device_id_type=MESH)
            greeted += 1

    for load in loads[1:6]:
        load.start()

    tile = (8, LANES)
    lane = iota(tile, 1)
    part = lane // SIDE
    def exchange(out, rec, sems, count):
        for d in range(1, group):
            peer = (me + d) % group
            pltpu.make_async_remote_copy(
                src_ref=out.at[peer, pl.ds(0, count)],
                dst_ref=rec.at[me, pl.ds(0, count)],
                send_sem=sems.at[0],
                recv_sem=sems.at[1],
                device_id=rank_id(peer),
                device_id_type=MESH,
            ).start()
        rec[me, pl.ds(0, count)] = out[me, pl.ds(0, count)]

    def all_of(out, rec, sems, count):
        most = pl.ds(0, group - 1)
        return pltpu.make_async_remote_copy(
            src_ref=out.at[most, pl.ds(0, count)],
            dst_ref=rec.at[most, pl.ds(0, count)],
            send_sem=sems.at[0],
            recv_sem=sems.at[1],
            device_id=rank_id((me + 1) % group),
            device_id_type=MESH,
        )

    def pack_parents():
        for s in range(slots):
            idx = box_col[s] * FOOT + (lane % FOOT)
            for m in range(FOOT // 4):
                acc = jnp.zeros(tile, jnp.float32)
                for k in range(4):
                    for h in range(2):
                        X = DEEP + 4 * m + k
                        a = P0[X, pl.ds(first + 8 * h, 8)]
                        for b in range(1, along_y):
                            other = P0[X, pl.ds(first + FOOT * b + 8 * h, 8)]
                            a = jnp.where(box_row[s] == b, other, a)
                        acc = jnp.where(lane // FOOT == 2 * k + h, take(a, idx), acc)
                compact[s, pl.ds(8 * m, 8), :] = acc

        for q in range(group):
            acc = jnp.zeros((32, LANES), jnp.float32)
            for s in range(slots):
                acc = jnp.where(owner[0, s] == q, compact[s], acc)
            pout[q, pl.ds(0, 32)] = acc

    def pack_flags():
        for q in range(group):
            flag = zero_tile
            for s in range(slots):
                flag = jnp.where(owner[0, s] == q, 1.0, flag)
            pout[q, pl.ds(32, 8)] = flag

    def slot_masks():
        count = zero_tile
        for q in range(group):
            flag = prec[q, pl.ds(32, 8)]
            slotid[q] = jnp.where(flag > 0.5, count, -1.0)
            count = count + flag
        return count

    def ghosts(par):
        tiles = []
        for m in range(FOOT // 4):
            at = pl.ds(8 * m, 8)
            for j in range(slots):
                acc = zero_tile
                for q in range(group):
                    acc = jnp.where(slotid[q] == float(j), prec[q, at], acc)
                tiles.append(acc)
        for k in range(4):
            for h in range(2):
                idx = k * 32 + h * FOOT + (lane % SIDE) // 2
                for m in range(FOOT // 4):
                    acc = take(tiles[m * slots], idx)
                    for j in range(1, slots):
                        acc = jnp.where(part == j, take(tiles[m * slots + j], idx), acc)
                    for e in range(2):
                        G[par, 4 * m + k, pl.ds(2 * 8 * h + e, 8, stride=2), :] = acc

    wide = (FCH, LANES)
    z_pos = iota(wide, 1) % SIDE

    def start_of(x):
        return 8 + (x + 1) * FPLANE

    def edges(par):
        for v in V:
            v[pl.ds(start_of(-1), SIDE)] = G[par, 0]
            v[pl.ds(start_of(SIDE), SIDE)] = G[par, FOOT - 1]
            for X in range(FOOT):
                low = G[par, X, pl.ds(0, 1)]
                top = G[par, X, pl.ds(SIDE - 1, 1)]
                for e in range(2):
                    v[pl.ds(start_of(2 * X + e) - 1, 1)] = low
                    v[pl.ds(start_of(2 * X + e) + SIDE, 1)] = top

    def beside_fine(v, par, x, r):
        at = start_of(x) + r
        u = v[pl.ds(at, FCH)]
        ghost = G[par, x // 2, pl.ds(r, FCH)]
        zu = jnp.where(z_pos < SIDE - 1, turn(u, -1), ghost)
        zl = jnp.where(z_pos > 0, turn(u, 1), ghost)
        across = v[pl.ds(at + FPLANE, FCH)] + v[pl.ds(at - FPLANE, FCH)]
        along = v[pl.ds(at + 1, FCH)] + v[pl.ds(at - 1, FCH)]
        return u, (across + along) + (zu + zl)

    def fine_sweep(vp, par):
        for x in range(SIDE):
            for r in range(0, SIDE, FCH):
                at = pl.ds(r, FCH)
                u, s = beside_fine(V[vp], par, x, r)
                V[1 - vp][pl.ds(start_of(x) + r, FCH)] = KEEP * u + FW[x, at] * (FS[x, at] + s)

    def fine_remainder(vp, par):
        total = jnp.zeros(wide, jnp.float32)
        for X in range(FOOT):
            for r in range(0, SIDE, FCH):
                at = pl.ds(r, FCH)
                t = None
                for e in range(2):
                    x = 2 * X + e
                    u, s = beside_fine(V[vp], par, x, r)
                    w = (FS[x, at] - FD[x, at] * u) + s
                    total = total + w * w
                    t = w if t is None else t + w
                T[X, at] = t
        square = zero_tile
        for g in range(FCH // 8):
            square = square + total[8 * g : 8 * g + 8]
        return square

    def shrink():
        for m in range(FOOT // 4):
            packed = []
            for k in range(4):
                X = 4 * m + k
                halves = []
                for h in range(2):
                    even = T[X, pl.ds(16 * h, 8, stride=2), :]
                    odd = T[X, pl.ds(16 * h + 1, 8, stride=2), :]
                    both = even + odd
                    halves.append(both + turn(both, -1))
                packed.append(jnp.where(lane % 2 == 0, halves[0], turn(halves[1], 1)) * 0.125)
            for j in range(slots):
                acc = turn(packed[0], -SIDE * j)
                for k in range(1, 4):
                    acc = jnp.where(part == k, turn(packed[k], SIDE * (k - j)), acc)
                R[j, pl.ds(8 * m, 8)] = acc

    def pack_returns():
        for q in range(group):
            which = slotid[q]
            for m in range(FOOT // 4):
                at = pl.ds(m * 8, 8)
                acc = zero_tile
                for j in range(slots):
                    acc = jnp.where(which == float(j), R[j, at], acc)
                rout[q, at] = acc

    def deposit():
        cols = [jnp.where(box_live[s], box_col[s], -1) for s in range(slots)]
        tiles = []
        for m in range(FOOT // 4):
            for s in range(slots):
                tiles.append(rrec[jnp.minimum(owner[0, s], group - 1), pl.ds(8 * m, 8)])
        for k in range(4):
            for h in range(2):
                idx = k * 32 + (lane % FOOT) * 2 + h
                for m in range(FOOT // 4):
                    got = []
                    for s in range(slots):
                        got.append(jnp.where(lane // FOOT == cols[s], take(tiles[m * slots + s], idx), 0.0))
                    for b in range(along_y):
                        x, y = 4 * m + k, FOOT * b + 8 * h
                        acc = c_src[x, pl.ds(y, 8)]
                        for s in range(slots):
                            acc = acc + jnp.where(box_row[s] == b, got[s], 0.0)
                        E0[DEEP + x, pl.ds(first + y, 8)] = acc

    def spread_row(row, received, sems, peers):
        for d, to in enumerate(peers):
            pltpu.make_async_remote_copy(
                src_ref=row,
                dst_ref=received.at[d],
                send_sem=sems.at[0],
                recv_sem=sems.at[1],
                device_id=to,
                device_id_type=MESH,
            ).start()

    def add_rows(row, received, sems):
        wait = pltpu.make_async_remote_copy(
            src_ref=received,
            dst_ref=received,
            send_sem=sems.at[0],
            recv_sem=sems.at[1],
            device_id=rank_id((me + 1) % group),
            device_id_type=MESH,
        )
        wait.wait_recv()
        wait.wait_send()
        total = row[...]
        for d in range(received.shape[0]):
            total = total + received[d]
        return total

    tall = iota((ny, LANES), 1)

    def pack_lanes(F, f):
        acc = turn(F[DEEP, inner], DEEP)
        for x in range(1, nx):
            acc = jnp.where(tall // (2 * DEEP) == x, turn(F[DEEP + x, inner], 2 * DEEP * x + DEEP), acc)
        pk[f] = acc

    def regions(fields, depth, d):
        dx, dy, dz = d
        x_src = {0: inside, -1: pl.ds(DEEP, depth), 1: pl.ds(DEEP + nx - depth, depth)}[dx]
        x_dst = {0: inside, -1: pl.ds(DEEP + nx, depth), 1: pl.ds(DEEP - depth, depth)}[dx]
        if dz == 0:
            y_src = {0: inner, -1: pl.ds(first, 8), 1: pl.ds(first + ny - 8, 8)}[dy]
            y_dst = {0: inner, -1: pl.ds(first + ny, 8), 1: pl.ds(PAD, 8)}[dy]
            return H0.at[fields, x_src, y_src], H0.at[fields, x_dst, y_dst]
        y_src = {0: pl.ds(0, ny), -1: pl.ds(0, 8), 1: pl.ds(ny - 8, 8)}[dy]
        y_dst = {0: pl.ds(8, ny), -1: pl.ds(8 + ny, 8), 1: pl.ds(0, 8)}[dy]
        return pk.at[fields, y_src], zs.at[fields, {0: 0, -1: 1, 1: 2}[dx], 0 if dz < 0 else 1, y_dst]

    def there(d):
        tests = []
        for step, at, count in zip(d, (gx, gy, gz), sizes):
            if step < 0:
                tests.append(at > 0)
            if step > 0:
                tests.append(at < count - 1)
        return functools.reduce(jnp.logical_and, tests)

    def flag(d):
        return tuple(abs(v) if n == 2 else v for v, n in zip(d, sizes))

    flags = sorted({flag(d) for d in DIRS})

    def halo_copy(kind, fields, depth, i):
        d = DIRS[i]
        source, target = regions(fields, depth, d)
        return pltpu.make_async_remote_copy(
            src_ref=source,
            dst_ref=target,
            send_sem=h_send.at[flags.index(flag(d))],
            recv_sem=h_recv.at[kind, flags.index(flag(tuple(-v for v in d)))],
            device_id=(gx + d[0], gy + d[1], gz + d[2]),
            device_id_type=MESH,
        )

    def halo_wait(kind, fields, depth, i):
        d = DIRS[i]
        _, target = regions(fields, depth, tuple(-v for v in d))
        return pltpu.make_async_remote_copy(
            src_ref=target,
            dst_ref=target,
            send_sem=h_send.at[flags.index(flag(d))],
            recv_sem=h_recv.at[kind, flags.index(flag(d))],
            device_id=(gx + d[0], gy + d[1], gz + d[2]),
            device_id_type=MESH,
        )

    def clear_halos():
        for d in DIRS:

            @pl.when(jnp.logical_not(there(d)))
            def _():
                _, target = regions(pl.ds(0, 3), DEEP, tuple(-v for v in d))
                target[...] = jnp.zeros(target.shape, jnp.float32)

    far_first = sorted(range(len(DIRS)), key=lambda i: -sum(map(abs, DIRS[i])))
    flat = [i for i in far_first if DIRS[i][2] == 0]
    packed = [i for i in far_first if DIRS[i][2] != 0]
    planes = [i for i in flat if DIRS[i][1] == 0]
    others = [i for i in far_first if i not in planes]

    def send_halo(kind, fields, depth, which):
        for i in which:
            pl.when(there(DIRS[i]))(halo_copy(kind, fields, depth, i).start)

    def wait_halo(kind, fields, depth):
        for i in reversed(far_first):

            @pl.when(there(DIRS[i]))
            def _():
                halo_copy(kind, fields, depth, i).wait_send()
                halo_wait(kind, fields, depth, i).wait_recv()

    both, only_start, only_composite = pl.ds(0, 2), pl.ds(0, 1), pl.ds(2, 1)

    low_part = iota((rows, LANES), 1) % (2 * DEEP) >= DEEP

    def lane_halo(f, depth):
        merged = [jnp.where(low_part, zs[f, a, 0], zs[f, a, 1]) for a in range(3)]
        for X in range(DEEP - depth, DEEP + nx + depth):
            if X < DEEP:
                a, i = 2, nx - DEEP + X
            elif X < DEEP + nx:
                a, i = 0, X - DEEP
            else:
                a, i = 1, X - DEEP - nx
            yield X, turn(merged[a], -(2 * DEEP * i + DEEP))

    def unpack_lanes(f, F1):
        for X, value in lane_halo(f, DEEP):
            F1[X, block] = value

    def reach(depth):
        for X in range(DEEP - depth, DEEP + nx + depth):
            left = depth - max(DEEP - X, X - (DEEP + nx - 1), 0)
            for r in range(PAD, PAD + rows, 8):
                rest = left - (0 if first <= r < first + ny else 1)
                if rest >= 0:
                    yield X, r, 2 if rest else 1

    lane0, lane127 = lane == 0, lane == LANES - 1

    def sweep(source, target, comp, depth, squares=False):
        U0, U1 = source
        total = zero_tile
        for X, r, tiles in reach(depth):
            here, up, down = pl.ds(r, 8), pl.ds(r + 1, 8), pl.ds(r - 1, 8)
            u = (U0[X, here], U1[X, here])
            prev = [turn(v, 1) for v in u]
            nxt = [turn(v, -1) for v in u]
            for t in range(tiles):
                U = source[t]
                z = jnp.where(lane0, prev[1 - t], prev[t]) + jnp.where(lane127, nxt[1 - t], nxt[t])
                s = ((U[X - 1, here] + U[X + 1, here]) + (U[X, up] + U[X, down])) + z
                if comp is not None:
                    s = s + comp[t][X, here]
                target[t][X, here] = KEEP * u[t] + (W0, W1)[t][X, here] * s
                if squares:
                    last = s - (6.0 + c_shift[X - DEEP, pl.ds(r - first, 8)]) * u[t]
                    total = total + last * last
        return total

    def inner_composite():
        for x in range(nx):
            X = DEEP + x
            A0[X, inner] = A0[X, inner] + W0[X, inner] * E0[X, inner]

    def outer_composite():
        values = dict(lane_halo(2, DEEP - 1))
        for X, r, tiles in reach(DEEP - 1):
            at = pl.ds(r, 8)
            inside_block = DEEP <= X < DEEP + nx and first <= r < first + ny
            if not inside_block:
                A0[X, at] = A0[X, at] + W0[X, at] * E0[X, at]
            if tiles == 2:
                value = values[X][r - PAD : r - PAD + 8]
                Q1[X, at] = value
                A1[X, at] = A1[X, at] + W1[X, at] * value

    loads[6].wait()
    loads[7].wait()
    box_row = []
    box_col = []
    box_live = []
    for s in range(slots):
        box_row.append((corner[1, 0, s] // 2 - gy * ny) // FOOT)
        box_col.append((corner[2, 0, s] // 2 - gz * nz) // FOOT)
        box_live.append(owner[0, s] < group)
    loads[0].wait()
    pack_parents()
    pack_flags()
    pl.semaphore_wait(barrier, greeted)
    exchange(pout, prec, p_sem, 40)
    clear_halos()
    for load in loads[1:6]:
        load.wait()
    for x in range(nx):
        W0[DEEP + x, inner] = OMEGA / (6.0 + c_shift[x])
    send_halo(0, both, DEEP, planes)

    def spread(a, x):
        parts = [a[pl.ds(x * 8 * slots + j, 8, stride=slots), :] for j in range(slots)]
        result = []
        for w in range(SIDE // 8):
            acc = turn(parts[0], -SIDE * w)
            for j in range(1, slots):
                acc = jnp.where(part == j, turn(parts[j], SIDE * (j - w)), acc)
            result.append(acc)
        return result

    def gather(parts):
        result = []
        for j in range(slots):
            acc = turn(parts[0], -SIDE * j)
            for w in range(1, SIDE // 8):
                acc = jnp.where(part == w, turn(parts[w], SIDE * (w - j)), acc)
            result.append(acc)
        return result

    def prepare():
        @pl.loop(0, SIDE, unroll=4)
        def _(x):
            for w, value in enumerate(spread(f_start, x)):
                V0[pl.ds(8 + (x + 1) * FPLANE + w, 8, stride=4), :] = value
            for w, value in enumerate(spread(f_src, x)):
                FS[x, pl.ds(w, 8, stride=4), :] = value
            for w, value in enumerate(spread(f_shift, x)):
                diagonal = 6.0 + value
                FD[x, pl.ds(w, 8, stride=4), :] = diagonal
                FW[x, pl.ds(w, 8, stride=4), :] = OMEGA / diagonal

    prepare()
    pack_lanes(P0, 0)
    pack_lanes(W0, 1)
    send_halo(0, both, DEEP, others)

    vp = 0
    for cycle in range(CYCLES):
        par = cycle % 2
        parents = all_of(pout, prec, p_sem, 32 if cycle else 40)
        parents.wait_recv()
        if cycle > 0:
            send_halo(0, only_start, DEEP, others)
        if cycle == 0:
            count = slot_masks()
            occupied = [count > float(j) for j in range(slots)]
            live_lanes = count > part.astype(jnp.float32)
        ghosts(par)
        if cycle > 0:
            for x in range(SIDE):
                at = pl.ds(start_of(x), SIDE)
                V[vp][at] = V[vp][at] + (G[par, x // 2] - G[1 - par, x // 2])
        edges(par)
        for _ in range(FSWEEPS):
            fine_sweep(vp, par)
            vp = 1 - vp
        square = jnp.where(live_lanes, fine_remainder(vp, par), 0.0)
        shrink()
        returns = all_of(rout, rrec, r_sem, 32)
        if cycle > 0:
            returns.wait_send()
        pack_returns()
        exchange(rout, rrec, r_sem, 32)
        wait_halo(0, only_start if cycle else both, DEEP)
        unpack_lanes(0, P1)
        if cycle == 0:
            unpack_lanes(1, W1)
        sweep((P0, P1), (A0, A1), None, DEEP - 1)
        returns.wait_recv()
        deposit()
        pack_lanes(E0, 2)
        send_halo(1, only_composite, DEEP - 1, far_first)
        inner_composite()
        wait_halo(1, only_composite, DEEP - 1)
        outer_composite()
        now, later = (A0, A1), (B0, B1)
        for depth in range(CSWEEPS - 2, 0, -1):
            sweep(now, later, (E0, Q1), depth)
            now, later = later, now
        total = sweep(now, (P0, None), (E0, None), 0, True)
        sums[cycle] = square + total
        parents.wait_send()
        if cycle == CYCLES - 1:
            halves = []
            for k in range(2):
                row = jnp.sum(sums[k], axis=0, keepdims=True)
                halves.append(row + turn(row, LANES // 2))
            own[...] = jnp.where(iota((1, LANES), 1) < LANES // 2, halves[0], halves[1])
            peers = []
            for a, b, c in itertools.product(range(n_gx), range(n_gy), range(n_gz)):
                if (a or b or c) and (direct or (b == 0 and c == 0)):
                    peers.append(((gx + a) % n_gx, (gy + b) % n_gy, (gz + c) % n_gz))
            spread_row(own, xsum, n_sem, peers)
        pack_parents()
        exchange(pout, prec, p_sem, 32)
        if cycle < CYCLES - 1:
            send_halo(0, only_start, DEEP, planes)
            pack_lanes(P0, 0)

    par = CYCLES % 2
    for x in range(nx):
        pot_out[x] = P0[DEEP + x, inner]

    def settle():
        @pl.loop(0, FOOT, unroll=4)
        def _(X):
            for e in range(2):
                x = 2 * X + e
                parts = []
                for w in range(SIDE // 8):
                    old = G[1 - par, X, pl.ds(w, 8, stride=4), :]
                    parts.append(V[vp][pl.ds(8 + (x + 1) * FPLANE + w, 8, stride=4), :] - old)
                for j, value in enumerate(gather(parts)):
                    PRE[x, j] = value

    settle()
    if not direct:
        team[...] = add_rows(own, xsum, n_sem)
        spread_row(team, gsum, g_sem, [rank_id((me + d) % group) for d in range(1, group)])

    returns.wait_send()
    parents = all_of(pout, prec, p_sem, 32)
    parents.wait_recv()
    parents.wait_send()
    ghosts(par)

    def deliver():
        for X in range(FOOT):
            parts = [G[par, X, pl.ds(w, 8, stride=4), :] for w in range(SIDE // 8)]
            for j, value in enumerate(gather(parts)):
                for e in range(2):
                    x = 2 * X + e
                    place = pl.ds(x * 8 * slots + j, 8, stride=slots)
                    fine_out[place, :] = jnp.where(occupied[j], PRE[x, j] + value, 0.0)

    deliver()
    whole = add_rows(own, xsum, n_sem) if direct else add_rows(team, gsum, g_sem)
    cells = float(nx * ny * nz * devices)
    mine = (lane >= LANES // 2) == (iota(tile, 0) > 0)
    both = jnp.where(mine, jnp.broadcast_to(whole, tile), 0.0)
    norm_out[...] = jnp.broadcast_to(jnp.sqrt(jnp.sum(both, axis=1, keepdims=True) / cells), tile)


def finish(norms, pot, rows, pot_out, rows_out, norm_out, held, sem):
    load = pltpu.make_async_copy(norms, held, sem.at[0])
    stores = [load]
    for k, (source, target) in enumerate(((rows, rows_out), (pot, pot_out))):
        count = source.shape[0] // PIECES
        for i in range(PIECES):
            at = pl.ds(i * count, count)
            stores.append(pltpu.make_async_copy(source.at[at], target.at[at], sem.at[1 + k * PIECES + i]))
    for store in stores:
        store.start()
    load.wait()
    for k in range(CYCLES):
        norm_out[k] = held[k, 0]
    for store in stores[1:]:
        store.wait()


def to_rows(a):
    slots, fine = a.shape
    return a.reshape(slots, fine // LANES, LANES).transpose(1, 0, 2).reshape(slots * fine // LANES, LANES)


def from_rows(a, slots):
    return a.reshape(-1, slots, LANES).transpose(1, 0, 2).reshape(slots, -1)


def local(sizes, c_src, c_shift, c_start, f_src, f_shift, f_start, corner, owner):
    n_gx, n_gy, n_gz = sizes
    group = n_gy * n_gz
    slots = owner.shape[1]
    nx, ny, nz = c_src.shape
    fine = f_src.shape[1]
    f32 = jnp.float32
    devices = n_gx * group
    direct = devices <= 64
    flags = math.prod(2 if n == 2 else 3 for n in sizes) - 1
    assert 2 * DEEP * nx == LANES == nz and slots * SIDE == LANES and nx == FOOT
    vmem = pl.BlockSpec(memory_space=pltpu.VMEM)
    smem = pl.BlockSpec(memory_space=pltpu.SMEM)
    anywhere = pl.BlockSpec(memory_space=pl.ANY)
    dma = pltpu.SemaphoreType.DMA
    rows = pltpu.VMEM((slots * fine // LANES, LANES), f32)
    ring = pltpu.VMEM((nx + 2 * DEEP, ny + 5 * 8, LANES), f32)
    box = pltpu.VMEM((8 + (SIDE + 2) * FPLANE + 8, LANES), f32)
    planes = pltpu.VMEM((SIDE, SIDE, LANES), f32)
    pot, fine_rows, norms = pl.pallas_call(
        functools.partial(kernel, sizes),
        out_shape=(pltpu.VMEM((nx, ny, nz), f32), rows, pltpu.VMEM((8, LANES), f32)),
        in_specs=[anywhere] * 8,
        out_specs=(vmem, vmem, vmem),
        scratch_shapes=[
            pltpu.SMEM((3, 1, slots), jnp.int32),
            pltpu.SMEM((1, slots), jnp.int32),
            pltpu.VMEM((nx, ny, nz), f32),
            pltpu.VMEM((nx, ny, nz), f32),
            rows,
            rows,
            rows,
            dma((8,)),
        ]
        + [pltpu.VMEM((3,) + ring.shape, f32)]
        + [ring] * 7
        + [
            pltpu.VMEM((3, ny, LANES), f32),
            pltpu.VMEM((3, 3, 2, ny + 16, LANES), f32),
            box,
            box,
            pltpu.VMEM((FOOT, SIDE, LANES), f32),
            planes,
            planes,
            planes,
            pltpu.VMEM((2, FOOT, SIDE, LANES), f32),
            pltpu.VMEM((SIDE, slots, 8, LANES), f32),
            pltpu.VMEM((slots, 32, LANES), f32),
            pltpu.VMEM((slots, 32, LANES), f32),
            pltpu.VMEM((group, 40, LANES), f32),
            pltpu.VMEM((group, 40, LANES), f32),
            pltpu.VMEM((group, 32, LANES), f32),
            pltpu.VMEM((group, 32, LANES), f32),
            pltpu.VMEM((group, 8, LANES), f32),
            pltpu.VMEM((CYCLES, 8, LANES), f32),
            pltpu.VMEM((1, LANES), f32),
            pltpu.VMEM((1, LANES), f32),
            pltpu.VMEM(((devices if direct else n_gx) - 1, 1, LANES), f32),
            pltpu.VMEM((group - 1, 1, LANES), f32),
            dma((2,)),
            dma((2,)),
            dma((flags,)),
            dma((2, flags)),
            dma((2,)),
            dma((2,)),
        ],
        compiler_params=pltpu.CompilerParams(collective_id=0, has_side_effects=True, vmem_limit_bytes=63000000),
    )(corner.transpose(2, 0, 1), owner, c_src, c_shift, c_start, to_rows(f_src), to_rows(f_shift), to_rows(f_start))
    pot, fine_rows, norms = pl.pallas_call(
        finish,
        out_shape=(
            jax.ShapeDtypeStruct(pot.shape, f32),
            jax.ShapeDtypeStruct(fine_rows.shape, f32),
            jax.ShapeDtypeStruct((CYCLES,), f32),
        ),
        in_specs=[vmem, vmem, vmem],
        out_specs=(anywhere, anywhere, smem),
        scratch_shapes=[pltpu.SMEM((8, LANES), f32), dma((1 + 2 * PIECES,))],
        compiler_params=pltpu.CompilerParams(vmem_limit_bytes=8 << 20),
    )(norms, pot, fine_rows)
    return pot, from_rows(fine_rows, slots), norms


def solution(mesh):
    sizes = (mesh.shape["gx"], mesh.shape["gy"], mesh.shape["gz"])
    everywhere = ("gx", "gy", "gz")
    block = P(*everywhere)
    in_specs = (
        block,
        block,
        block,
        P(everywhere, None),
        P(everywhere, None),
        P(everywhere, None),
        P(everywhere, None, None),
        P(everywhere, None),
    )
    out_specs = (block, P(everywhere, None), P())
    return jax.shard_map(
        functools.partial(local, sizes), mesh=mesh, in_specs=in_specs, out_specs=out_specs, check_vma=False
    )
```

```python
import functools
import itertools

import jax
import jax.numpy as jnp
from jax import lax
from jax.experimental import pallas as pl
from jax.experimental.pallas import tpu as pltpu
from jax.sharding import PartitionSpec as P

FOOT = 16
CYCLES = 2
CSWEEPS = 4
FSWEEPS = 3
OMEGA = 0.8
KEEP = 1.0 - OMEGA
MESH = pl.DeviceIdType.MESH
LANES = 128
SIDE = 2 * FOOT
DEEP = CSWEEPS
PAD = 8
CH = 16
PIECES = 2
FCH = 16
FPLANE = SIDE + 8


def take(x, idx):
    return jnp.take_along_axis(x, idx, axis=1, mode="promise_in_bounds")


def iota(shape, dim):
    return lax.broadcasted_iota(jnp.int32, shape, dim)


def directions(sizes):
    z_steps = (0, 1) if sizes[2] == 2 else (-1, 0, 1)
    return [d for d in itertools.product((-1, 0, 1), (-1, 0, 1), z_steps) if any(d)]


def turn(x, by):
    by = by % LANES
    return pltpu.roll(x, by, 1) if by else x


def kernel(
    sizes,
    corner_hbm,
    owner_hbm,
    c_src_hbm,
    c_shift_hbm,
    c_start_hbm,
    f_src_hbm,
    f_shift_hbm,
    f_start_hbm,
    pot_out,
    fine_out,
    norm_out,
    corner,
    owner,
    c_src,
    c_shift,
    f_src,
    f_shift,
    f_start,
    H0,
    P1,
    W1,
    A0,
    A1,
    B0,
    B1,
    Q1,
    pk,
    zs,
    V0,
    V1,
    T,
    FW,
    FS,
    FD,
    G,
    PRE,
    compact,
    R,
    pout,
    prec,
    rout,
    rrec,
    slotid,
    sums,
    own,
    team,
    xsum,
    gsum,
    p_sem,
    r_sem,
    h_send,
    h_recv,
    n_sem,
    g_sem,
):
    n_gx, n_gy, n_gz = sizes
    group = n_gy * n_gz
    devices = n_gx * group
    direct = devices <= 64
    slots = owner_hbm.shape[1]
    nx, ny, nz = c_src_hbm.shape
    along_y = ny // FOOT
    first, rows = PAD + 8, ny + 16
    inner, block = pl.ds(first, ny), pl.ds(PAD, rows)
    inside = pl.ds(DEEP, nx)
    gx, gy, gz = lax.axis_index("gx"), lax.axis_index("gy"), lax.axis_index("gz")
    me = gy * n_gz + gz
    DIRS = directions(sizes)
    pair = sizes[2] == 2
    V = (V0, V1)
    P0, W0, E0 = (H0.at[f] for f in range(3))
    zero_rows = jnp.zeros((rows, LANES), jnp.float32)
    zero_tile = jnp.zeros((8, LANES), jnp.float32)

    def rank_id(rank):
        return (gx, rank // n_gz, rank % n_gz)

    loads = [
        pltpu.make_async_copy(source, target, h_send.at[i])
        for i, (source, target) in enumerate(
            (
                (c_start_hbm, H0.at[0, inside, inner]),
                (c_shift_hbm, c_shift),
                (c_src_hbm, c_src),
                (f_start_hbm, f_start),
                (f_src_hbm, f_src),
                (f_shift_hbm, f_shift),
                (corner_hbm, corner),
                (owner_hbm, owner),
            )
        )
    ]
    for load in (loads[0], loads[6], loads[7]):
        load.start()

    barrier = pltpu.get_barrier_semaphore()
    greeted = 0
    for a, b, c in itertools.product(range(n_gx), range(n_gy), range(n_gz)):
        near = [min(v, n - v) for v, n in zip((a, b, c), sizes)]
        if any(near) and (direct or a == 0 or (b == 0 and c == 0) or max(near) == 1):
            other = ((gx + a) % n_gx, (gy + b) % n_gy, (gz + c) % n_gz)
            pl.semaphore_signal(barrier, inc=1, device_id=other, device_id_type=MESH)
            greeted += 1

    for load in loads[1:6]:
        load.start()

    tile = (8, LANES)
    lane = iota(tile, 1)
    part = lane // SIDE
    def exchange(out, rec, sems, count):
        for d in range(1, group):
            peer = (me + d) % group
            pltpu.make_async_remote_copy(
                src_ref=out.at[peer, pl.ds(0, count)],
                dst_ref=rec.at[me, pl.ds(0, count)],
                send_sem=sems.at[0],
                recv_sem=sems.at[1],
                device_id=rank_id(peer),
                device_id_type=MESH,
            ).start()
        rec[me, pl.ds(0, count)] = out[me, pl.ds(0, count)]

    def all_of(out, rec, sems, count):
        most = pl.ds(0, group - 1)
        return pltpu.make_async_remote_copy(
            src_ref=out.at[most, pl.ds(0, count)],
            dst_ref=rec.at[most, pl.ds(0, count)],
            send_sem=sems.at[0],
            recv_sem=sems.at[1],
            device_id=rank_id((me + 1) % group),
            device_id_type=MESH,
        )

    def pack_parents():
        for s in range(slots):
            idx = box_col[s] * FOOT + (lane % FOOT)
            for m in range(FOOT // 4):
                acc = jnp.zeros(tile, jnp.float32)
                for k in range(4):
                    for h in range(2):
                        X = DEEP + 4 * m + k
                        a = P0[X, pl.ds(first + 8 * h, 8)]
                        for b in range(1, along_y):
                            other = P0[X, pl.ds(first + FOOT * b + 8 * h, 8)]
                            a = jnp.where(box_row[s] == b, other, a)
                        acc = jnp.where(lane // FOOT == 2 * k + h, take(a, idx), acc)
                compact[s, pl.ds(8 * m, 8), :] = acc

        for q in range(group):
            acc = jnp.zeros((32, LANES), jnp.float32)
            for s in range(slots):
                acc = jnp.where(owner[0, s] == q, compact[s], acc)
            pout[q, pl.ds(0, 32)] = acc

    def pack_flags():
        for q in range(group):
            flag = zero_tile
            for s in range(slots):
                flag = jnp.where(owner[0, s] == q, 1.0, flag)
            pout[q, pl.ds(32, 8)] = flag

    def slot_masks():
        count = zero_tile
        for q in range(group):
            flag = prec[q, pl.ds(32, 8)]
            slotid[q] = jnp.where(flag > 0.5, count, -1.0)
            count = count + flag
        return count

    def ghosts(par):
        tiles = []
        for m in range(FOOT // 4):
            at = pl.ds(8 * m, 8)
            for j in range(slots):
                acc = zero_tile
                for q in range(group):
                    acc = jnp.where(slotid[q] == float(j), prec[q, at], acc)
                tiles.append(acc)
        for k in range(4):
            for h in range(2):
                idx = k * 32 + h * FOOT + (lane % SIDE) // 2
                for m in range(FOOT // 4):
                    acc = take(tiles[m * slots], idx)
                    for j in range(1, slots):
                        acc = jnp.where(part == j, take(tiles[m * slots + j], idx), acc)
                    for e in range(2):
                        G[par, 4 * m + k, pl.ds(2 * 8 * h + e, 8, stride=2), :] = acc

    wide = (FCH, LANES)
    z_pos = iota(wide, 1) % SIDE

    def start_of(x):
        return 8 + (x + 1) * FPLANE

    def edges(par):
        for v in V:
            v[pl.ds(start_of(-1), SIDE)] = G[par, 0]
            v[pl.ds(start_of(SIDE), SIDE)] = G[par, FOOT - 1]
            for X in range(FOOT):
                low = G[par, X, pl.ds(0, 1)]
                top = G[par, X, pl.ds(SIDE - 1, 1)]
                for e in range(2):
                    v[pl.ds(start_of(2 * X + e) - 1, 1)] = low
                    v[pl.ds(start_of(2 * X + e) + SIDE, 1)] = top

    def beside_fine(cells, v, par, x, r):
        def cell(x):
            if (x, r) not in cells:
                cells[x, r] = v[pl.ds(start_of(x) + r, FCH)]
            return cells[x, r]

        at = start_of(x) + r
        u = cell(x)
        ghost = G[par, x // 2, pl.ds(r, FCH)]
        zu = jnp.where(z_pos < SIDE - 1, turn(u, -1), ghost)
        zl = jnp.where(z_pos > 0, turn(u, 1), ghost)
        along = v[pl.ds(at + 1, FCH)] + v[pl.ds(at - 1, FCH)]
        return u, ((cell(x + 1) + cell(x - 1)) + along) + (zu + zl)

    def fine_sweep(vp, par):
        cells = {}
        for r in range(0, SIDE, FCH):
            at = pl.ds(r, FCH)
            for x in range(SIDE):
                u, s = beside_fine(cells, V[vp], par, x, r)
                V[1 - vp][pl.ds(start_of(x) + r, FCH)] = KEEP * u + FW[x, at] * (FS[x, at] + s)

    def fine_remainder(vp, par):
        cells = {}
        total = jnp.zeros(wide, jnp.float32)
        for r in range(0, SIDE, FCH):
            at = pl.ds(r, FCH)
            for X in range(FOOT):
                t = None
                for e in range(2):
                    x = 2 * X + e
                    u, s = beside_fine(cells, V[vp], par, x, r)
                    w = (FS[x, at] - FD[x, at] * u) + s
                    total = total + w * w
                    t = w if t is None else t + w
                T[X, at] = t
        square = zero_tile
        for g in range(FCH // 8):
            square = square + total[8 * g : 8 * g + 8]
        return square

    def shrink():
        for m in range(FOOT // 4):
            packed = []
            for k in range(4):
                X = 4 * m + k
                halves = []
                for h in range(2):
                    even = T[X, pl.ds(16 * h, 8, stride=2), :]
                    odd = T[X, pl.ds(16 * h + 1, 8, stride=2), :]
                    pairs = even + odd
                    halves.append(pairs + turn(pairs, 1 if h else -1))
                packed.append(jnp.where(lane % 2 == 0, halves[0], halves[1]) * 0.125)
            for j in range(slots):
                acc = turn(packed[0], -SIDE * j)
                for k in range(1, 4):
                    acc = jnp.where(part == k, turn(packed[k], SIDE * (k - j)), acc)
                R[j, pl.ds(8 * m, 8)] = acc

    def pack_returns():
        for q in range(group):
            which = slotid[q]
            for m in range(FOOT // 4):
                at = pl.ds(m * 8, 8)
                acc = zero_tile
                for j in range(slots):
                    acc = jnp.where(which == float(j), R[j, at], acc)
                rout[q, at] = acc

    def deposit():
        cols = [jnp.where(box_live[s], box_col[s], -1) for s in range(slots)]
        tiles = []
        for m in range(FOOT // 4):
            for s in range(slots):
                tiles.append(rrec[jnp.minimum(owner[0, s], group - 1), pl.ds(8 * m, 8)])
        for k in range(4):
            for h in range(2):
                idx = k * 32 + (lane % FOOT) * 2 + h
                for m in range(FOOT // 4):
                    got = []
                    for s in range(slots):
                        got.append(jnp.where(lane // FOOT == cols[s], take(tiles[m * slots + s], idx), 0.0))
                    for b in range(along_y):
                        x, y = 4 * m + k, FOOT * b + 8 * h
                        acc = c_src[x, pl.ds(y, 8)]
                        for s in range(slots):
                            acc = acc + jnp.where(box_row[s] == b, got[s], 0.0)
                        E0[DEEP + x, pl.ds(first + y, 8)] = acc

    def spread_row(row, received, sems, peers):
        for d, to in enumerate(peers):
            pltpu.make_async_remote_copy(
                src_ref=row,
                dst_ref=received.at[d],
                send_sem=sems.at[0],
                recv_sem=sems.at[1],
                device_id=to,
                device_id_type=MESH,
            ).start()

    def add_rows(row, received, sems):
        wait = pltpu.make_async_remote_copy(
            src_ref=received,
            dst_ref=received,
            send_sem=sems.at[0],
            recv_sem=sems.at[1],
            device_id=rank_id((me + 1) % group),
            device_id_type=MESH,
        )
        wait.wait_recv()
        wait.wait_send()
        total = row[...]
        for d in range(received.shape[0]):
            total = total + received[d]
        return total

    tall = iota((ny, LANES), 1)

    def pack_lanes(F, f):
        acc = turn(F[DEEP, inner], DEEP)
        for x in range(1, nx):
            acc = jnp.where(tall // (2 * DEEP) == x, turn(F[DEEP + x, inner], 2 * DEEP * x + DEEP), acc)
        pk[f] = acc

    def sent_from(fields, depth, d):
        dx, dy, dz = d
        if dz == 0:
            x_src = {0: inside, -1: pl.ds(DEEP, depth), 1: pl.ds(DEEP + nx - depth, depth)}[dx]
            y_src = {0: inner, -1: pl.ds(first, 8), 1: pl.ds(first + ny - 8, 8)}[dy]
            return H0.at[fields, x_src, y_src]
        return pk.at[fields, {0: pl.ds(0, ny), -1: pl.ds(0, 8), 1: pl.ds(ny - 8, 8)}[dy]]

    def lands_at(fields, depth, d, z_side):
        dx, dy, dz = d
        if dz == 0:
            x_dst = {0: inside, 1: pl.ds(DEEP + nx, depth), -1: pl.ds(DEEP - depth, depth)}[dx]
            y_dst = {0: inner, 1: pl.ds(first + ny, 8), -1: pl.ds(PAD, 8)}[dy]
            return H0.at[fields, x_dst, y_dst]
        y_dst = {0: pl.ds(8, ny), 1: pl.ds(8 + ny, 8), -1: pl.ds(0, 8)}[dy]
        return zs.at[fields, {0: 0, 1: 1, -1: 2}[dx], z_side, y_dst]

    def back(d):
        return (-d[0], -d[1], d[2] if pair else -d[2])

    def device(d):
        return (gx + d[0], gy + d[1], (1 - gz if d[2] else gz) if pair else gz + d[2])

    def own_side(d):
        return gz if pair else (0 if d[2] > 0 else 1)

    def their_side(d):
        return 1 - gz if pair else (0 if d[2] < 0 else 1)

    def there(d):
        tests = []
        for step, at, count in zip(d[:2] if pair else d, (gx, gy, gz), sizes):
            if step < 0:
                tests.append(at > 0)
            if step > 0:
                tests.append(at < count - 1)
        return functools.reduce(jnp.logical_and, tests) if tests else None

    def when_there(d):
        test = there(d)
        return (lambda f: f()) if test is None else pl.when(test)

    def halo_copy(kind, fields, depth, i):
        d = DIRS[i]
        return pltpu.make_async_remote_copy(
            src_ref=sent_from(fields, depth, d),
            dst_ref=lands_at(fields, depth, back(d), their_side(d)),
            send_sem=h_send.at[i],
            recv_sem=h_recv.at[kind, DIRS.index(back(d))],
            device_id=device(d),
            device_id_type=MESH,
        )

    def halo_wait(kind, fields, depth, i):
        d = DIRS[i]
        target = lands_at(fields, depth, d, own_side(d))
        return pltpu.make_async_remote_copy(
            src_ref=target,
            dst_ref=target,
            send_sem=h_send.at[i],
            recv_sem=h_recv.at[kind, i],
            device_id=device(d),
            device_id_type=MESH,
        )

    def clear_halos():
        for d in DIRS:
            if there(d) is not None:

                @pl.when(jnp.logical_not(there(d)))
                def _():
                    target = lands_at(pl.ds(0, 3), DEEP, d, own_side(d))
                    target[...] = jnp.zeros(target.shape, jnp.float32)

        if pair:
            for f in range(3):
                for a in range(3):
                    zs[f, a, 1 - gz] = zero_rows

    far_first = sorted(range(len(DIRS)), key=lambda i: -sum(map(abs, DIRS[i])))
    flat = [i for i in far_first if DIRS[i][2] == 0]
    packed = [i for i in far_first if DIRS[i][2] != 0]
    planes = [i for i in flat if DIRS[i][1] == 0]
    others = [i for i in far_first if i not in planes]

    def send_halo(kind, fields, depth, which):
        for i in which:
            when_there(DIRS[i])(halo_copy(kind, fields, depth, i).start)

    def wait_halo(kind, fields, depth):
        for i in reversed(far_first):

            @when_there(DIRS[i])
            def _():
                halo_copy(kind, fields, depth, i).wait_send()
                halo_wait(kind, fields, depth, i).wait_recv()

    both, only_start, only_composite = pl.ds(0, 2), pl.ds(0, 1), pl.ds(2, 1)

    low_part = iota((rows, LANES), 1) % (2 * DEEP) >= DEEP

    def lane_halo(f, depth):
        merged = [jnp.where(low_part, zs[f, a, 0], zs[f, a, 1]) for a in range(3)]
        for X in range(DEEP - depth, DEEP + nx + depth):
            if X < DEEP:
                a, i = 2, nx - DEEP + X
            elif X < DEEP + nx:
                a, i = 0, X - DEEP
            else:
                a, i = 1, X - DEEP - nx
            yield X, turn(merged[a], -(2 * DEEP * i + DEEP))

    def unpack_lanes(f, F1):
        for X, value in lane_halo(f, DEEP):
            F1[X, block] = value

    def reach(depth):
        for r in range(PAD, PAD + rows, 8):
            for X in range(DEEP - depth, DEEP + nx + depth):
                left = depth - max(DEEP - X, X - (DEEP + nx - 1), 0)
                rest = left - (0 if first <= r < first + ny else 1)
                if rest >= 0:
                    yield X, r, 2 if rest else 1

    lane0, lane127 = lane == 0, lane == LANES - 1

    def sweep(source, target, comp, depth, squares=False):
        total = zero_tile
        cells = {}

        def cell(t, X, r):
            if (t, X, r) not in cells:
                cells[t, X, r] = source[t][X, pl.ds(r, 8)]
            return cells[t, X, r]

        for X, r, tiles in reach(depth):
            here, up, down = pl.ds(r, 8), pl.ds(r + 1, 8), pl.ds(r - 1, 8)
            u = (cell(0, X, r), cell(1, X, r))
            if tiles == 2:
                prev = [turn(v, 1) for v in u]
                nxt = [turn(v, -1) for v in u]
            for t in range(tiles):
                U = source[t]
                if tiles == 2:
                    z = jnp.where(lane0, prev[1 - t], prev[t]) + jnp.where(lane127, nxt[1 - t], nxt[t])
                else:
                    z = turn(jnp.where(lane127, u[1], u[0]), 1) + turn(jnp.where(lane0, u[1], u[0]), -1)
                s = ((cell(t, X - 1, r) + cell(t, X + 1, r)) + (U[X, up] + U[X, down])) + z
                if comp is not None:
                    s = s + comp[t][X, here]
                target[t][X, here] = KEEP * u[t] + (W0, W1)[t][X, here] * s
                if squares:
                    last = s - (6.0 + c_shift[X - DEEP, pl.ds(r - first, 8)]) * u[t]
                    total = total + last * last
        return total

    def inner_composite():
        for x in range(nx):
            X = DEEP + x
            A0[X, inner] = A0[X, inner] + W0[X, inner] * E0[X, inner]

    def outer_composite():
        values = dict(lane_halo(2, DEEP - 1))
        for X, r, tiles in reach(DEEP - 1):
            at = pl.ds(r, 8)
            inside_block = DEEP <= X < DEEP + nx and first <= r < first + ny
            if not inside_block:
                A0[X, at] = A0[X, at] + W0[X, at] * E0[X, at]
            if tiles == 2:
                value = values[X][r - PAD : r - PAD + 8]
                Q1[X, at] = value
                A1[X, at] = A1[X, at] + W1[X, at] * value

    loads[6].wait()
    loads[7].wait()
    box_row = []
    box_col = []
    box_live = []
    for s in range(slots):
        box_row.append((corner[1, 0, s] // 2 - gy * ny) // FOOT)
        box_col.append((corner[2, 0, s] // 2 - gz * nz) // FOOT)
        box_live.append(owner[0, s] < group)
    loads[0].wait()
    pack_parents()
    pack_flags()
    pl.semaphore_wait(barrier, greeted)
    exchange(pout, prec, p_sem, 40)
    clear_halos()
    for load in loads[1:6]:
        load.wait()
    for x in range(nx):
        W0[DEEP + x, inner] = OMEGA / (6.0 + c_shift[x])
    send_halo(0, both, DEEP, planes)

    def spread(a, x):
        parts = [a[pl.ds(x * 8 * slots + j, 8, stride=slots), :] for j in range(slots)]
        result = []
        for w in range(SIDE // 8):
            acc = turn(parts[0], -SIDE * w)
            for j in range(1, slots):
                acc = jnp.where(part == j, turn(parts[j], SIDE * (j - w)), acc)
            result.append(acc)
        return result

    def gather(parts):
        result = []
        for j in range(slots):
            acc = turn(parts[0], -SIDE * j)
            for w in range(1, SIDE // 8):
                acc = jnp.where(part == w, turn(parts[w], SIDE * (w - j)), acc)
            result.append(acc)
        return result

    def prepare():
        @pl.loop(0, SIDE, unroll=4)
        def _(x):
            for w, value in enumerate(spread(f_start, x)):
                V0[pl.ds(8 + (x + 1) * FPLANE + w, 8, stride=4), :] = value
            for w, value in enumerate(spread(f_src, x)):
                FS[x, pl.ds(w, 8, stride=4), :] = value
            for w, value in enumerate(spread(f_shift, x)):
                diagonal = 6.0 + value
                FD[x, pl.ds(w, 8, stride=4), :] = diagonal
                FW[x, pl.ds(w, 8, stride=4), :] = OMEGA / diagonal

    prepare()
    pack_lanes(P0, 0)
    pack_lanes(W0, 1)
    send_halo(0, both, DEEP, others)

    vp = 0
    for cycle in range(CYCLES):
        par = cycle % 2
        parents = all_of(pout, prec, p_sem, 32 if cycle else 40)
        parents.wait_recv()
        if cycle > 0:
            send_halo(0, only_start, DEEP, others)
        if cycle == 0:
            count = slot_masks()
            occupied = [count > float(j) for j in range(slots)]
            live_lanes = count > part.astype(jnp.float32)
        ghosts(par)
        if cycle > 0:
            for x in range(SIDE):
                at = pl.ds(start_of(x), SIDE)
                V[vp][at] = V[vp][at] + (G[par, x // 2] - G[1 - par, x // 2])
        edges(par)
        for _ in range(FSWEEPS):
            fine_sweep(vp, par)
            vp = 1 - vp
        square = jnp.where(live_lanes, fine_remainder(vp, par), 0.0)
        shrink()
        returns = all_of(rout, rrec, r_sem, 32)
        if cycle > 0:
            returns.wait_send()
        pack_returns()
        exchange(rout, rrec, r_sem, 32)
        wait_halo(0, only_start if cycle else both, DEEP)
        unpack_lanes(0, P1)
        if cycle == 0:
            unpack_lanes(1, W1)
        sweep((P0, P1), (A0, A1), None, DEEP - 1)
        returns.wait_recv()
        deposit()
        pack_lanes(E0, 2)
        send_halo(1, only_composite, DEEP - 1, far_first)
        inner_composite()
        wait_halo(1, only_composite, DEEP - 1)
        outer_composite()
        now, later = (A0, A1), (B0, B1)
        for depth in range(CSWEEPS - 2, 0, -1):
            sweep(now, later, (E0, Q1), depth)
            now, later = later, now
        total = sweep(now, (P0, None), (E0, None), 0, True)
        sums[cycle] = square + total
        parents.wait_send()
        if cycle == CYCLES - 1:
            halves = []
            for k in range(2):
                row = jnp.sum(sums[k], axis=0, keepdims=True)
                halves.append(row + turn(row, LANES // 2))
            own[...] = jnp.where(iota((1, LANES), 1) < LANES // 2, halves[0], halves[1])
            peers = []
            for a, b, c in itertools.product(range(n_gx), range(n_gy), range(n_gz)):
                if (a or b or c) and (direct or (b == 0 and c == 0)):
                    peers.append(((gx + a) % n_gx, (gy + b) % n_gy, (gz + c) % n_gz))
            spread_row(own, xsum, n_sem, peers)
        pack_parents()
        exchange(pout, prec, p_sem, 32)
        if cycle < CYCLES - 1:
            send_halo(0, only_start, DEEP, planes)
            pack_lanes(P0, 0)

    par = CYCLES % 2
    for x in range(nx):
        pot_out[x] = P0[DEEP + x, inner]

    def settle():
        @pl.loop(0, FOOT, unroll=4)
        def _(X):
            for e in range(2):
                x = 2 * X + e
                parts = []
                for w in range(SIDE // 8):
                    old = G[1 - par, X, pl.ds(w, 8, stride=4), :]
                    parts.append(V[vp][pl.ds(8 + (x + 1) * FPLANE + w, 8, stride=4), :] - old)
                for j, value in enumerate(gather(parts)):
                    PRE[x, j] = value

    settle()
    if not direct:
        team[...] = add_rows(own, xsum, n_sem)
        spread_row(team, gsum, g_sem, [rank_id((me + d) % group) for d in range(1, group)])

    returns.wait_send()
    parents = all_of(pout, prec, p_sem, 32)
    parents.wait_recv()
    parents.wait_send()
    ghosts(par)

    def deliver():
        for X in range(FOOT):
            parts = [G[par, X, pl.ds(w, 8, stride=4), :] for w in range(SIDE // 8)]
            for j, value in enumerate(gather(parts)):
                for e in range(2):
                    x = 2 * X + e
                    place = pl.ds(x * 8 * slots + j, 8, stride=slots)
                    fine_out[place, :] = jnp.where(occupied[j], PRE[x, j] + value, 0.0)

    deliver()
    whole = add_rows(own, xsum, n_sem) if direct else add_rows(team, gsum, g_sem)
    cells = float(nx * ny * nz * devices)
    mine = (lane >= LANES // 2) == (iota(tile, 0) > 0)
    both = jnp.where(mine, jnp.broadcast_to(whole, tile), 0.0)
    norm_out[...] = jnp.broadcast_to(jnp.sqrt(jnp.sum(both, axis=1, keepdims=True) / cells), tile)


def finish(norms, pot, rows, pot_out, rows_out, norm_out, held, sem):
    load = pltpu.make_async_copy(norms, held, sem.at[0])
    stores = [load]
    for k, (source, target) in enumerate(((rows, rows_out), (pot, pot_out))):
        count = source.shape[0] // PIECES
        for i in range(PIECES):
            at = pl.ds(i * count, count)
            stores.append(pltpu.make_async_copy(source.at[at], target.at[at], sem.at[1 + k * PIECES + i]))
    for store in stores:
        store.start()
    load.wait()
    for k in range(CYCLES):
        norm_out[k] = held[k, 0]
    for store in stores[1:]:
        store.wait()


def to_rows(a):
    slots, fine = a.shape
    return a.reshape(slots, fine // LANES, LANES).transpose(1, 0, 2).reshape(slots * fine // LANES, LANES)


def from_rows(a, slots):
    return a.reshape(-1, slots, LANES).transpose(1, 0, 2).reshape(slots, -1)


def local(sizes, c_src, c_shift, c_start, f_src, f_shift, f_start, corner, owner):
    n_gx, n_gy, n_gz = sizes
    group = n_gy * n_gz
    slots = owner.shape[1]
    nx, ny, nz = c_src.shape
    fine = f_src.shape[1]
    f32 = jnp.float32
    devices = n_gx * group
    direct = devices <= 64
    flags = len(directions(sizes))
    assert 2 * DEEP * nx == LANES == nz and slots * SIDE == LANES and nx == FOOT
    vmem = pl.BlockSpec(memory_space=pltpu.VMEM)
    smem = pl.BlockSpec(memory_space=pltpu.SMEM)
    anywhere = pl.BlockSpec(memory_space=pl.ANY)
    dma = pltpu.SemaphoreType.DMA
    rows = pltpu.VMEM((slots * fine // LANES, LANES), f32)
    ring = pltpu.VMEM((nx + 2 * DEEP, ny + 5 * 8, LANES), f32)
    box = pltpu.VMEM((8 + (SIDE + 2) * FPLANE + 8, LANES), f32)
    planes = pltpu.VMEM((SIDE, SIDE, LANES), f32)
    pot, fine_rows, norms = pl.pallas_call(
        functools.partial(kernel, sizes),
        out_shape=(pltpu.VMEM((nx, ny, nz), f32), rows, pltpu.VMEM((8, LANES), f32)),
        in_specs=[anywhere] * 8,
        out_specs=(vmem, vmem, vmem),
        scratch_shapes=[
            pltpu.SMEM((3, 1, slots), jnp.int32),
            pltpu.SMEM((1, slots), jnp.int32),
            pltpu.VMEM((nx, ny, nz), f32),
            pltpu.VMEM((nx, ny, nz), f32),
            rows,
            rows,
            rows,
        ]
        + [pltpu.VMEM((3,) + ring.shape, f32)]
        + [ring] * 7
        + [
            pltpu.VMEM((3, ny, LANES), f32),
            pltpu.VMEM((3, 3, 2, ny + 16, LANES), f32),
            box,
            box,
            pltpu.VMEM((FOOT, SIDE, LANES), f32),
            planes,
            planes,
            planes,
            pltpu.VMEM((2, FOOT, SIDE, LANES), f32),
            pltpu.VMEM((SIDE, slots, 8, LANES), f32),
            pltpu.VMEM((slots, 32, LANES), f32),
            pltpu.VMEM((slots, 32, LANES), f32),
            pltpu.VMEM((group, 40, LANES), f32),
            pltpu.VMEM((group, 40, LANES), f32),
            pltpu.VMEM((group, 32, LANES), f32),
            pltpu.VMEM((group, 32, LANES), f32),
            pltpu.VMEM((group, 8, LANES), f32),
            pltpu.VMEM((CYCLES, 8, LANES), f32),
            pltpu.VMEM((1, LANES), f32),
            pltpu.VMEM((1, LANES), f32),
            pltpu.VMEM(((devices if direct else n_gx) - 1, 1, LANES), f32),
            pltpu.VMEM((group - 1, 1, LANES), f32),
            dma((2,)),
            dma((2,)),
            dma((flags,)),
            dma((2, flags)),
            dma((2,)),
            dma((2,)),
        ],
        compiler_params=pltpu.CompilerParams(collective_id=0, has_side_effects=True, vmem_limit_bytes=63000000),
    )(corner.transpose(2, 0, 1), owner, c_src, c_shift, c_start, to_rows(f_src), to_rows(f_shift), to_rows(f_start))
    pot, fine_rows, norms = pl.pallas_call(
        finish,
        out_shape=(
            jax.ShapeDtypeStruct(pot.shape, f32),
            jax.ShapeDtypeStruct(fine_rows.shape, f32),
            jax.ShapeDtypeStruct((CYCLES,), f32),
        ),
        in_specs=[vmem, vmem, vmem],
        out_specs=(anywhere, anywhere, smem),
        scratch_shapes=[pltpu.SMEM((8, LANES), f32), dma((1 + 2 * PIECES,))],
        compiler_params=pltpu.CompilerParams(vmem_limit_bytes=8 << 20),
    )(norms, pot, fine_rows)
    return pot, from_rows(fine_rows, slots), norms


def solution(mesh):
    sizes = (mesh.shape["gx"], mesh.shape["gy"], mesh.shape["gz"])
    everywhere = ("gx", "gy", "gz")
    block = P(*everywhere)
    in_specs = (
        block,
        block,
        block,
        P(everywhere, None),
        P(everywhere, None),
        P(everywhere, None),
        P(everywhere, None, None),
        P(everywhere, None),
    )
    out_specs = (block, P(everywhere, None), P())
    return jax.shard_map(
        functools.partial(local, sizes), mesh=mesh, in_specs=in_specs, out_specs=out_specs, check_vma=False
    )
```
